256 devices in a mesh: seq: 64 (over x, y, z_lo, core), tp: 4 (over z_hi).
Axes of the slice: x: 4, y: 4, z: 8 (z_hi: 4, z_lo: 2; z = z_hi * 2 + z_lo), core: 2. Of those that a mesh axis runs over, the one named last changes fastest.
Arguments:
- hidden_in: bfloat16 [32768, 2048], P('seq', 'tp'), may hold values from -60 to 60
- w_query: bfloat16 [2048, 2048], P(None, 'tp'), may hold values from -0.125 to 0.125
- w_key: bfloat16 [2048, 2048], P(None, 'tp'), may hold values from -0.125 to 0.125
- w_value: bfloat16 [2048, 2048], P(None, 'tp'), may hold values from -0.8984375 to 0.8984375
- w_pos: bfloat16 [2048, 2048], P(None, 'tp'), may hold values from -0.125 to 0.125
- w_out: bfloat16 [2048, 2048], P('tp'), may hold values from -0.125 to 0.125
- bias_content: float32 [16, 128], P('tp'), may hold values from -4 to 4
- bias_pos: float32 [16, 128], P('tp'), may hold values from -4 to 4
- norm_gain: float32 [2048], P('tp'), may hold values from 0.1 to 1.9
- norm_bias: float32 [2048], P('tp'), may hold values from -3 to 3
Outputs:
- hidden_out: bfloat16 [32768, 2048], P('seq', 'tp')
The draws below stay inside these ranges and needn't reach their ends.
All inputs are finite; a program needn't handle non-finite values.
Results may differ from the reference program's by a relative error of at most 0.014.
The reference program's roundings to bfloat16 on the way count: a program that leaves them out, or rounds other values in their place, can miss the bound.
Values may be sent and summed in bfloat16 or wider, within the bound.
A program may use at most 128 MiB of HBM per device.

```python
import jax
import jax.numpy as jnp
from jax import lax

D = 2048
HEADS = 16
HEAD_DIM = 128
SEG = 512
TOKENS = 32768
N_SEQ = 64
N_TP = 4


def draw_hidden_in(key, part):
    first, second, third = jax.random.split(key, 3)
    base = jax.random.normal(first, (TOKENS, D), jnp.float32)
    columns = jnp.exp(jnp.log(3.0) * jnp.arange(D).astype(jnp.float32) / D)
    columns = columns * jax.random.uniform(second, (D,), jnp.float32, minval=0.7, maxval=1.4)
    rows = jnp.exp(jax.random.uniform(third, (TOKENS, 1), jnp.float32, minval=0.0, maxval=jnp.log(2.0)))
    value = base * rows * columns[None, :]
    return jnp.clip(value, -60.0, 60.0).astype(jnp.bfloat16)


def levels(own_key, dims, pieces, least, top_value):
    def one(dim, parts):
        heights = jax.random.uniform(jax.random.fold_in(jax.random.fold_in(own_key, 6), dim), (parts,), jnp.float32, least / len(pieces), top_value / len(pieces))
        return jnp.repeat(jnp.exp(heights), dims[dim] // parts).reshape((-1,) + (1,) * (len(dims) - dim - 1))

    gain = one(*pieces[0])
    for cut in pieces[1:]:
        gain = gain * one(*cut)
    return gain


def scatter_about(own_key, extent, deviation, bound, shards=(), held_as=jnp.bfloat16):
    values = jax.random.normal(own_key, extent, jnp.float32) * deviation
    if len(shards) > 0:
        values = levels(own_key, extent, shards, -0.22, 0.18) * values
    return jnp.clip(values, min=-bound, max=bound).astype(held_as)


def setup_inputs(seed: int = 0) -> dict:
    splits = jax.random.split(jax.random.key(seed), 11)
    hidden_in = draw_hidden_in(jax.random.fold_in(splits[10], 71), 0)
    w_query = scatter_about(splits[1], (D, HEADS * HEAD_DIM), D ** -0.5, 0.125, ((1, 4),))
    w_key = scatter_about(splits[2], (D, HEADS * HEAD_DIM), D ** -0.5, 0.125, ((1, 4),))
    w_value = scatter_about(splits[3], (D, HEADS * HEAD_DIM), 0.15, 0.8984375, ((1, 4),))
    w_pos = scatter_about(splits[4], (D, HEADS * HEAD_DIM), D ** -0.5, 0.125, ((1, 4),))
    w_out = scatter_about(splits[5], (HEADS * HEAD_DIM, D), (HEADS * HEAD_DIM) ** -0.5, 0.125, ((0, 4),))
    bias_content = scatter_about(splits[6], (HEADS, HEAD_DIM), 1.0, 4.0, ((0, 4),), jnp.float32)
    bias_pos = scatter_about(splits[7], (HEADS, HEAD_DIM), 1.0, 4.0, ((0, 4),), jnp.float32)
    norm_gain = jnp.clip(1.0 + 0.18 * jax.random.normal(splits[8], (D,), jnp.float32), 0.1, 1.9)
    norm_bias = scatter_about(splits[9], (D,), 0.5, 3.0, ((0, 4),), jnp.float32)
    return dict(hidden_in=hidden_in, w_query=w_query, w_key=w_key, w_value=w_value, w_pos=w_pos, w_out=w_out, bias_content=bias_content, bias_pos=bias_pos, norm_gain=norm_gain, norm_bias=norm_bias)


def relative_table(span, width):
    half = width // 2
    freq = jnp.exp(-jnp.log(10000.0) * jnp.arange(half).astype(jnp.float32) / half)
    distance = (span - 1 - jnp.arange(span)).astype(jnp.float32)
    angle = distance[:, None] * freq[None, :]
    return jnp.concatenate([jnp.sin(angle), jnp.cos(angle)], 1).astype(jnp.bfloat16)

def shift_rows(table, seg, span):
    heads = table.shape[0]
    padded = jnp.pad(table, ((0, 0), (0, 0), (0, 1)))
    flat = padded.reshape(heads, seg * (span + 1))
    return flat[:, seg - 1:seg - 1 + seg * span].reshape(heads, seg, span)

def reference(hidden_in, w_query, w_key, w_value, w_pos, w_out, bias_content, bias_pos, norm_gain, norm_bias):
    span = 3 * SEG
    memory = 2 * SEG
    width = HEADS * HEAD_DIM
    query = jnp.dot(hidden_in, w_query, preferred_element_type=jnp.float32).astype(jnp.bfloat16)
    keys = jnp.dot(hidden_in, w_key, preferred_element_type=jnp.float32).astype(jnp.bfloat16)
    values = jnp.dot(hidden_in, w_value, preferred_element_type=jnp.float32).astype(jnp.bfloat16)
    rel = jnp.dot(relative_table(span, D), w_pos, preferred_element_type=jnp.float32).astype(jnp.bfloat16)
    rel = rel.reshape(span, HEADS, HEAD_DIM).astype(jnp.float32)
    front = jnp.zeros((memory, width), jnp.bfloat16)
    pad_keys = jnp.concatenate([front, keys], 0)
    pad_values = jnp.concatenate([front, values], 0)
    scale = 1.0 / jnp.sqrt(jnp.float32(HEAD_DIM))

    def one_segment(index):
        start = (index * SEG).astype(jnp.int32)
        q_rows = lax.dynamic_slice_in_dim(query, start, SEG, 0).astype(jnp.float32).reshape(SEG, HEADS, HEAD_DIM)
        k_rows = lax.dynamic_slice_in_dim(pad_keys, start, span, 0).astype(jnp.float32).reshape(span, HEADS, HEAD_DIM)
        v_rows = lax.dynamic_slice_in_dim(pad_values, start, span, 0).astype(jnp.float32).reshape(span, HEADS, HEAD_DIM)
        content_q = (q_rows + bias_content[None]).astype(jnp.bfloat16).astype(jnp.float32)
        pos_q = (q_rows + bias_pos[None]).astype(jnp.bfloat16).astype(jnp.float32)
        content = jnp.einsum('ihd,jhd->hij', content_q, k_rows)
        position = shift_rows(jnp.einsum('ihd,ehd->hie', pos_q, rel), SEG, span)
        score = (content + position) * scale
        row = jnp.arange(SEG)[:, None]
        col = jnp.arange(span)[None, :]
        allowed = (col <= row + memory) & (start - memory + col >= 0)
        score = jnp.where(allowed[None], score, jnp.float32(-1e+30))
        probs = jax.nn.softmax(score, axis=-1).astype(jnp.bfloat16).astype(jnp.float32)
        attended = jnp.einsum('hij,jhd->ihd', probs, v_rows)
        return attended.astype(jnp.bfloat16).reshape(SEG, width)
    attended = lax.map(one_segment, jnp.arange(N_SEQ).astype(jnp.int32)).reshape(TOKENS, width)
    group = width // N_TP
    branch = jnp.zeros((TOKENS, D), jnp.float32)
    for part in range(N_TP):
        piece = jnp.dot(attended[:, part * group:(part + 1) * group], w_out[part * group:(part + 1) * group], preferred_element_type=jnp.float32)
        branch = branch + piece.astype(jnp.bfloat16).astype(jnp.float32)
    summed = hidden_in.astype(jnp.float32) + branch
    center = lax.optimization_barrier(jnp.mean(summed, axis=1, keepdims=True))
    spread = lax.optimization_barrier(jnp.mean((summed - center) ** 2, axis=1, keepdims=True))
    normed = (summed - center) / jnp.sqrt(spread + 1e-05)
    return (normed * norm_gain[None] + norm_bias[None]).astype(jnp.bfloat16)
```

```python
import functools
import math

import jax
import jax.numpy as jnp
from jax import lax
from jax.experimental import pallas as pl
from jax.experimental.pallas import tpu as pltpu
from jax.sharding import PartitionSpec as P

MESH = pl.DeviceIdType.MESH
F32 = jnp.float32
BF16 = jnp.bfloat16
SEG = 512
ROWS = 128
CHUNKS = SEG // ROWS
HALF = ROWS // 2
WIDTH = 512
MODEL = 2048
HEAD = 128
FINE = 32
NEG = -1e30


def dot(a, b):
    return jnp.dot(a, b, preferred_element_type=F32)


def dot_t(a, b):
    return lax.dot_general(a, b, (((1,), (1,)), ((), ())), preferred_element_type=F32)


def copy_to(src, dst, sems, at, device):
    return pltpu.make_async_remote_copy(
        src_ref=src,
        dst_ref=dst,
        send_sem=sems[0].at[at],
        recv_sem=sems[1].at[at],
        device_id=device,
        device_id_type=MESH,
    )


def kernel(
    n_seq,
    hid, wq_in, wk_in, wv_in, wp_in, wo_in, bc, bp, gain, shift, out,
    g, wq, wkv, wp, wo, kv, cq, pq, rel, fine, coarse, att,
    opp, near_r, near_l, own, half_r, half_l, fin_r, fin_l, y, st_out, st_in,
    loc, up_s, up_r, dn_s, dn_r, y_s, y_r, d_s, d_r,
    or_s, or_r, ol_s, ol_r, fr_s, fr_r, fl_s, fl_r, st_s, st_r,
):
    s = lax.axis_index("seq")
    t = lax.axis_index("tp")
    core = lax.rem(s, 2)
    low = lax.rem(s // 2, 2)
    z = 2 * t + low
    right, left, across = lax.rem(t + 1, 4), lax.rem(t + 3, 4), lax.rem(t + 2, 4)
    mate = s + 2 - 4 * low
    up = (mate, lax.rem(t + low, 4))
    down = (mate, lax.rem(t + 3 + low, 4))
    twin = (s + 1 - 2 * core, t)
    to_right, to_left, to_across = (s, right), (s, left), (s, across)
    front = low == 0
    has_next = jnp.logical_and(front, s + 4 < n_seq)
    has_prev = jnp.logical_and(front, s >= 4)
    next_line = (lax.rem(s + 4, n_seq), t)
    prev_line = (lax.rem(s + n_seq - 4, n_seq), t)

    barrier = pltpu.get_barrier_semaphore()
    for device in (up, down, twin, to_right, to_left, to_across, next_line, prev_line):
        pl.semaphore_signal(barrier, inc=1, device_id=device, device_id_type=MESH)

    own_cols = pl.ds(pl.multiple_of(t * WIDTH, WIDTH), WIDTH)
    loads = [
        pltpu.make_async_copy(hid, g.at[low, :, own_cols], loc.at[0]),
        pltpu.make_async_copy(wp_in, wp, loc.at[1]),
        pltpu.make_async_copy(wk_in, wkv.at[:, pl.ds(0, WIDTH)], loc.at[2]),
        pltpu.make_async_copy(wv_in, wkv.at[:, pl.ds(WIDTH, WIDTH)], loc.at[3]),
        pltpu.make_async_copy(wq_in, wq, loc.at[4]),
    ]
    for c in range(4):
        loads.append(pltpu.make_async_copy(wo_in.at[:, pl.ds(c * WIDTH, WIDTH)], wo.at[c], loc.at[5 + c]))
    for load in loads:
        load.start()

    pl.semaphore_wait(barrier, 8)
    loads[0].wait()

    def block(z_from, r):
        cols = pl.ds(pl.multiple_of((z_from // 2) * WIDTH, WIDTH), WIDTH)
        return g.at[lax.rem(z_from, 2), pl.ds(r * ROWS, ROWS), cols]

    reach_up = [4 if r % 2 == 0 else 3 for r in range(CHUNKS)]
    reach_down = [7 - reach_up[r] for r in range(CHUNKS)]

    def send_up(r, d):
        ref = block(lax.rem(z + 8 - d, 8), r)
        return copy_to(ref, ref, (up_s, up_r), (d, r), up)

    def send_down(r, d):
        ref = block(lax.rem(z + d, 8), r)
        return copy_to(ref, ref, (dn_s, dn_r), (d, r), down)

    def came_up(r, d):
        ref = block(lax.rem(z + 8 - d, 8), r)
        return copy_to(ref, ref, (up_s, up_r), (d - 1, r), down)

    def came_down(r, d):
        ref = block(lax.rem(z + d, 8), r)
        return copy_to(ref, ref, (dn_s, dn_r), (d - 1, r), up)

    def tables():
        k = lax.broadcasted_iota(jnp.int32, (FINE, MODEL // 2), 1).astype(F32)
        freq = jnp.exp(k * (-math.log(10000.0) / (MODEL // 2)))
        row = lax.broadcasted_iota(jnp.int32, (FINE, MODEL // 2), 0)
        angle = (FINE - 1 - row).astype(F32) * freq
        fine[0] = jnp.sin(angle)
        fine[1] = jnp.cos(angle)
        n = 3 * SEG // FINE
        for part in range(n // 16):
            row = lax.broadcasted_iota(jnp.int32, (16, MODEL // 2), 0) + part * 16
            angle = (FINE * (n - 1 - row)).astype(F32) * freq[:16]
            coarse[0, part * 16 : part * 16 + 16, :] = jnp.sin(angle)
            coarse[1, part * 16 : part * 16 + 16, :] = jnp.cos(angle)

    def rel_rows(first, count):
        @pl.loop(first, first + count)
        def _(c):
            at = pl.multiple_of(c * 8, 8)
            sa, ca = coarse[0, pl.ds(at, 8), :], coarse[1, pl.ds(at, 8), :]
            sf, cf = fine[0], fine[1]
            sines, cosines = [], []
            for b in range(8):
                sb, cb = sa[b : b + 1], ca[b : b + 1]
                sines.append((sb * cf + cb * sf).astype(BF16))
                cosines.append((cb * cf - sb * sf).astype(BF16))
            half = MODEL // 2
            total = dot(jnp.concatenate(sines, 0), wp[:half]) + dot(jnp.concatenate(cosines, 0), wp[half:])
            rel[pl.ds(pl.multiple_of(c * 256, 256), 256), :] = total.astype(BF16)

    other_slot = jnp.where(front, 3, 0)

    def kv_rows(slot, r):
        return pl.ds(pl.multiple_of(slot * SEG + r * ROWS, ROWS), ROWS)

    def shift_line(r):
        return copy_to(kv.at[kv_rows(3, r)], kv.at[kv_rows(0, r)], (y_s, y_r), r, next_line)

    def shift_line_in(r):
        return copy_to(kv.at[kv_rows(3, r)], kv.at[kv_rows(0, r)], (y_s, y_r), r, prev_line)

    def to_twin(slot, r):
        return copy_to(kv.at[kv_rows(slot, r)], kv.at[kv_rows(1, r)], (d_s, d_r), r, twin)

    def project(r):
        rows = pl.ds(r * ROWS, ROWS)
        mine = g[low, rows, :]
        both = jnp.concatenate([mine, g[1 - low, rows, :]], 0)
        made = dot(both, wkv[...]).astype(BF16)
        kv[kv_rows(2, r), :] = made[:ROWS]
        kv[kv_rows(other_slot, r), :] = made[ROWS:]

        @pl.when(has_next)
        def _():
            shift_line(r).start()

        @pl.when(core == 0)
        def _():
            to_twin(2, r).start()

        @pl.when(jnp.logical_and(core == 1, low == 1))
        def _():
            to_twin(0, r).start()

        q = dot(mine, wq[...]).astype(BF16).astype(F32)
        for h in range(4):
            cols = slice(h * HEAD, (h + 1) * HEAD)
            cq[r * ROWS : (r + 1) * ROWS, cols] = (q[:, cols] + bc[h : h + 1, :]).astype(BF16)
            pq[r * ROWS : (r + 1) * ROWS, cols] = (q[:, cols] + bp[h : h + 1, :]).astype(BF16)

    @pl.when(jnp.logical_and(front, s < 4))
    def _():
        kv[0:SEG, :] = jnp.zeros((SEG, 2 * WIDTH), BF16)

    rel[3 * SEG :, :] = jnp.zeros((ROWS, WIDTH), BF16)

    side = {0: tables, 1: lambda: (loads[1].wait(), rel_rows(0, 2)), 3: lambda: rel_rows(2, 2), 5: lambda: rel_rows(4, 2)}
    last = CHUNKS - 1 + 2 * 4
    for key in range(last + 1):
        for d in range(5):
            r = key - 2 * d
            if r < 0 or r >= CHUNKS:
                continue
            if d == 0:
                send_up(r, 0).start()
                send_down(r, 0).start()
                continue
            if d <= reach_up[r]:
                came_up(r, d).wait_recv()
                if d < reach_up[r]:
                    send_up(r, d).start()
            if d <= reach_down[r]:
                came_down(r, d).wait_recv()
                if d < reach_down[r]:
                    send_down(r, d).start()
        if key in side:
            side[key]()
        if key >= 8:
            if key == 8:
                for load in loads[2:5]:
                    load.wait()
            project(key - 8)

    for r in range(CHUNKS):
        @pl.when(has_prev)
        def _():
            shift_line_in(r).wait_recv()

        @pl.when(jnp.logical_and(core == 1, front))
        def _():
            to_twin(0, r).start()

    for r in range(CHUNKS):
        to_twin(0, r).wait_recv()
    for load in loads[5:]:
        load.wait()

    start = jnp.maximum(2 * SEG - SEG * s, 0)
    scale = math.log2(math.e) / math.sqrt(HEAD)

    def attend(r):
        i0 = r * ROWS
        keys = 2 * SEG + ROWS + i0
        span = keys + ROWS
        e0 = SEG - ROWS - i0
        outside = jnp.where(lax.broadcasted_iota(jnp.int32, (1, keys), 1) >= start, 0.0, NEG).astype(F32)
        causal = lax.broadcasted_iota(jnp.int32, (ROWS, ROWS), 1) <= lax.broadcasted_iota(jnp.int32, (ROWS, ROWS), 0)

        def one(h):
            cols = pl.ds(pl.multiple_of(h * HEAD, HEAD), HEAD)
            vcols = pl.ds(pl.multiple_of(WIDTH + h * HEAD, HEAD), HEAD)
            content = dot_t(cq[i0 : i0 + ROWS, cols], kv[0:keys, cols])
            position = dot_t(pq[i0 : i0 + ROWS, cols], rel[e0 : e0 + span, cols])
            position = pltpu.roll(position, span - (ROWS - 1), 1, stride=1, stride_axis=0)[:, :keys]
            score = content + position + outside
            tail = jnp.where(causal, score[:, keys - ROWS :], NEG)
            score = jnp.concatenate([score[:, : keys - ROWS], tail], 1)
            top = jnp.max(score, axis=1, keepdims=True)
            e = jnp.exp2((score - top) * scale)
            norm = 1.0 / jnp.sum(e, axis=1, keepdims=True)
            att[i0 : i0 + ROWS, cols] = dot((e * norm).astype(BF16), kv[0:keys, vcols]).astype(BF16)

        @pl.loop(0, 2)
        def _(pair):
            one(2 * pair)
            one(2 * pair + 1)

    def opp_right(r):
        return copy_to(opp.at[r, pl.ds(0, HALF)], half_r.at[r], (or_s, or_r), r, to_right)

    def opp_left(r):
        return copy_to(opp.at[r, pl.ds(HALF, HALF)], half_l.at[r], (ol_s, ol_r), r, to_left)

    def fin_right(r):
        return copy_to(near_r.at[r], fin_r.at[r], (fr_s, fr_r), r, to_right)

    def fin_left(r):
        return copy_to(near_l.at[r], fin_l.at[r], (fl_s, fl_r), r, to_left)

    def output(r):
        a = att[r * ROWS : (r + 1) * ROWS, :]
        opp[r] = dot(a, wo[across]).astype(BF16)
        opp_right(r).start()
        opp_left(r).start()
        near_r[r] = dot(a, wo[right]).astype(BF16)
        near_l[r] = dot(a, wo[left]).astype(BF16)
        own[r] = dot(a, wo[t]).astype(BF16)

    def pass_on(r):
        opp_right(r).wait_recv()
        near_r[r, :HALF, :] = (near_r[r, :HALF, :].astype(F32) + half_r[r].astype(F32)).astype(BF16)
        fin_right(r).start()
        opp_left(r).wait_recv()
        near_l[r, HALF:, :] = (near_l[r, HALF:, :].astype(F32) + half_l[r].astype(F32)).astype(BF16)
        fin_left(r).start()

    others = (to_right, to_across, to_left)

    def stats_to(i, r):
        return copy_to(st_out.at[r], st_in.at[i, r], (st_s, st_r), (i, r), others[i])

    def collect(r):
        fin_right(r).wait_recv()
        fin_left(r).wait_recv()
        rows = pl.ds(r * ROWS, ROWS)
        total = g[low, rows, own_cols].astype(F32) + (
            own[r].astype(F32) + fin_r[r].astype(F32) + fin_l[r].astype(F32)
        )
        y[r] = total
        mean = jnp.sum(total, axis=1, keepdims=True) * (1.0 / WIDTH)
        centred = total - mean
        square = jnp.sum(centred * centred, axis=1, keepdims=True)
        lane = lax.broadcasted_iota(jnp.int32, (ROWS, 128), 1)
        both = jnp.where(lane == 0, mean, jnp.where(lane == 1, square, 0.0))
        st_out[r] = both.T[:8, :]
        for i in range(3):
            stats_to(i, r).start()

    def finish(r):
        for i in range(3):
            stats_to(i, r).wait_recv()
        stack = jnp.concatenate(
            [st_out[r], st_in[0, r], st_in[1, r], st_in[2, r], jnp.zeros((96, 128), F32)], 0
        ).T
        means = [stack[:, 8 * i : 8 * i + 1] for i in range(4)]
        squares = [stack[:, 8 * i + 1 : 8 * i + 2] for i in range(4)]
        mean = (means[0] + means[1] + means[2] + means[3]) * 0.25
        square = squares[0] + squares[1] + squares[2] + squares[3]
        for m in means:
            square = square + WIDTH * ((m - mean) * (m - mean))
        factor = lax.rsqrt(square * (1.0 / MODEL) + 1e-05)
        normed = (y[r] - mean) * factor
        out[r * ROWS : (r + 1) * ROWS, :] = (normed * gain[...] + shift[...]).astype(BF16)

    for r in range(CHUNKS):
        attend(r)
        output(r)
        if r >= 1:
            pass_on(r - 1)
        if r >= 2:
            collect(r - 2)
    pass_on(CHUNKS - 1)
    collect(CHUNKS - 2)
    for r in range(CHUNKS - 1):
        finish(r)
    collect(CHUNKS - 1)
    finish(CHUNKS - 1)

    for r in range(CHUNKS):
        for d in range(4):
            if d < reach_up[r]:
                send_up(r, d).wait_send()
            if d < reach_down[r]:
                send_down(r, d).wait_send()

        @pl.when(has_next)
        def _():
            shift_line(r).wait_send()

        to_twin(0, r).wait_send()
        for copy in (opp_right(r), opp_left(r), fin_right(r), fin_left(r)):
            copy.wait_send()
        for i in range(3):
            stats_to(i, r).wait_send()


def layer(n_seq, hidden_in, w_query, w_key, w_value, w_pos, w_out, bias_content, bias_pos, norm_gain, norm_bias):
    anywhere = pl.BlockSpec(memory_space=pl.ANY)
    vmem = pl.BlockSpec(memory_space=pltpu.VMEM)
    dma = pltpu.SemaphoreType.DMA
    per_chunk = [dma((CHUNKS,))] * 2
    return pl.pallas_call(
        functools.partial(kernel, n_seq),
        out_shape=jax.ShapeDtypeStruct((SEG, WIDTH), BF16),
        in_specs=[anywhere] * 6 + [vmem] * 4,
        out_specs=vmem,
        scratch_shapes=[
            pltpu.VMEM((2, SEG, MODEL), BF16),
            pltpu.VMEM((MODEL, WIDTH), BF16),
            pltpu.VMEM((MODEL, 2 * WIDTH), BF16),
            pltpu.VMEM((MODEL, WIDTH), BF16),
            pltpu.VMEM((4, WIDTH, WIDTH), BF16),
            pltpu.VMEM((4 * SEG, 2 * WIDTH), BF16),
            pltpu.VMEM((SEG, WIDTH), BF16),
            pltpu.VMEM((SEG, WIDTH), BF16),
            pltpu.VMEM((3 * SEG + ROWS, WIDTH), BF16),
            pltpu.VMEM((2, FINE, MODEL // 2), F32),
            pltpu.VMEM((2, 3 * SEG // FINE, MODEL // 2), F32),
            pltpu.VMEM((SEG, WIDTH), BF16),
            pltpu.VMEM((CHUNKS, ROWS, WIDTH), BF16),
            pltpu.VMEM((CHUNKS, ROWS, WIDTH), BF16),
            pltpu.VMEM((CHUNKS, ROWS, WIDTH), BF16),
            pltpu.VMEM((CHUNKS, ROWS, WIDTH), BF16),
            pltpu.VMEM((CHUNKS, HALF, WIDTH), BF16),
            pltpu.VMEM((CHUNKS, HALF, WIDTH), BF16),
            pltpu.VMEM((CHUNKS, ROWS, WIDTH), BF16),
            pltpu.VMEM((CHUNKS, ROWS, WIDTH), BF16),
            pltpu.VMEM((CHUNKS, ROWS, WIDTH), F32),
            pltpu.VMEM((CHUNKS, 8, 128), F32),
            pltpu.VMEM((3, CHUNKS, 8, 128), F32),
            dma((9,)),
            dma((4, CHUNKS)), dma((4, CHUNKS)), dma((4, CHUNKS)), dma((4, CHUNKS)),
            *per_chunk, *per_chunk, *per_chunk, *per_chunk, *per_chunk, *per_chunk,
            dma((3, CHUNKS)), dma((3, CHUNKS)),
        ],
        compiler_params=pltpu.CompilerParams(
            collective_id=0, has_side_effects=True, vmem_limit_bytes=60 * 2**20
        ),
    )(
        hidden_in, w_query, w_key, w_value, w_pos, w_out, bias_content, bias_pos,
        norm_gain.reshape(1, WIDTH), norm_bias.reshape(1, WIDTH),
    )


def solution(mesh):
    in_specs = (
        P("seq", "tp"),
        P(None, "tp"),
        P(None, "tp"),
        P(None, "tp"),
        P(None, "tp"),
        P("tp", None),
        P("tp", None),
        P("tp", None),
        P("tp"),
        P("tp"),
    )
    return jax.shard_map(
        functools.partial(layer, mesh.shape["seq"]),
        mesh=mesh,
        in_specs=in_specs,
        out_specs=P("seq", "tp"),
        check_vma=False,
    )
```

```python
import functools
import math

import jax
import jax.numpy as jnp
from jax import lax
from jax.experimental import pallas as pl
from jax.experimental.pallas import tpu as pltpu
from jax.sharding import PartitionSpec as P

MESH = pl.DeviceIdType.MESH
F32 = jnp.float32
BF16 = jnp.bfloat16
SEG = 512
ROWS = 128
CHUNKS = SEG // ROWS
HALF = ROWS // 2
PIECE = 64
PIECES = SEG // PIECE
WIDTH = 512
MODEL = 2048
HEAD = 128
FINE = 32
NEG = -1e30


def dot(a, b):
    return jnp.dot(a, b, preferred_element_type=F32)


def dot_t(a, b):
    return lax.dot_general(a, b, (((1,), (1,)), ((), ())), preferred_element_type=F32)


def copy_to(src, dst, sems, at, device):
    return pltpu.make_async_remote_copy(
        src_ref=src,
        dst_ref=dst,
        send_sem=sems[0].at[at],
        recv_sem=sems[1].at[at],
        device_id=device,
        device_id_type=MESH,
    )


def gather_order(slot=1.4, latency=3.6, weight=0.5):
    events = []
    done = [0.0] * PIECES
    for way, reach in enumerate(REACH):
        clock, ends = 0.0, {}
        left = [(p, d) for p in range(PIECES) for d in range(reach[p])]
        while left:
            ready = {(p, d): 0.0 if d == 0 else ends[p, d - 1] + latency for p, d in left if d == 0 or (p, d - 1) in ends}
            clock = max(clock, min(ready.values()))
            pick = min((x for x in ready if ready[x] <= clock + 1e-9), key=lambda x: (weight * x[0] - reach[x[0]] + x[1], x[0]))
            left.remove(pick)
            events.append((clock, way, *pick))
            clock += slot
            ends[pick] = clock
        for p in range(PIECES):
            done[p] = max(done[p], ends[p, reach[p] - 1] + latency)
    for c in range(CHUNKS):
        per = ROWS // PIECE
        events.append((max(done[c * per : (c + 1) * per]), 2, c, 0))
    return sorted(events)


REACH = ([4 if p % 2 == 0 else 3 for p in range(PIECES)], [3 if p % 2 == 0 else 4 for p in range(PIECES)])


def kernel(
    n_seq,
    hid, wq_in, wk_in, wv_in, wp_in, wo_in, bc, bp, gain, shift, out,
    g, wq, wkv, wp, wo, kv, cq, pq, rel, fine, coarse, att,
    opp, near_r, near_l, own, half_r, half_l, fin_r, fin_l, y, st_out, st_in,
    loc, up_s, up_r, dn_s, dn_r, y_s, y_r, d_s, d_r,
    or_s, or_r, ol_s, ol_r, fr_s, fr_r, fl_s, fl_r, st_s, st_r,
):
    s = lax.axis_index("seq")
    t = lax.axis_index("tp")
    core = lax.rem(s, 2)
    low = lax.rem(s // 2, 2)
    z = 2 * t + low
    right, left, across = lax.rem(t + 1, 4), lax.rem(t + 3, 4), lax.rem(t + 2, 4)
    mate = s + 2 - 4 * low
    up = (mate, lax.rem(t + low, 4))
    down = (mate, lax.rem(t + 3 + low, 4))
    twin = (s + 1 - 2 * core, t)
    to_right, to_left, to_across = (s, right), (s, left), (s, across)
    front = low == 0
    has_next = jnp.logical_and(front, s + 4 < n_seq)
    has_prev = jnp.logical_and(front, s >= 4)
    next_line = (lax.rem(s + 4, n_seq), t)
    prev_line = (lax.rem(s + n_seq - 4, n_seq), t)

    barrier = pltpu.get_barrier_semaphore()
    for device in (up, down, twin, to_right, to_left, to_across, next_line, prev_line):
        pl.semaphore_signal(barrier, inc=1, device_id=device, device_id_type=MESH)

    own_cols = pl.ds(pl.multiple_of(t * WIDTH, WIDTH), WIDTH)
    loads = [
        pltpu.make_async_copy(hid, g.at[low, :, own_cols], loc.at[0]),
        pltpu.make_async_copy(wp_in, wp, loc.at[1]),
        pltpu.make_async_copy(wk_in, wkv.at[:, pl.ds(0, WIDTH)], loc.at[2]),
        pltpu.make_async_copy(wv_in, wkv.at[:, pl.ds(WIDTH, WIDTH)], loc.at[3]),
        pltpu.make_async_copy(wq_in, wq, loc.at[4]),
    ]
    for c in range(4):
        loads.append(pltpu.make_async_copy(wo_in.at[:, pl.ds(c * WIDTH, WIDTH)], wo.at[c], loc.at[5 + c]))
    for load in loads:
        load.start()

    def block(z_from, p):
        cols = pl.ds(pl.multiple_of((z_from // 2) * WIDTH, WIDTH), WIDTH)
        return g.at[lax.rem(z_from, 2), pl.ds(p * PIECE, PIECE), cols]

    def send(way, p, d):
        ref = block(lax.rem(z + d, 8) if way else lax.rem(z + 8 - d, 8), p)
        return copy_to(ref, ref, (dn_s, dn_r) if way else (up_s, up_r), (d, p), down if way else up)

    def came(way, p, d):
        ref = block(lax.rem(z + d, 8) if way else lax.rem(z + 8 - d, 8), p)
        return copy_to(ref, ref, (dn_s, dn_r) if way else (up_s, up_r), (d - 1, p), up if way else down)

    def tables():
        k = lax.broadcasted_iota(jnp.int32, (FINE, MODEL // 2), 1).astype(F32)
        freq = jnp.exp(k * (-math.log(10000.0) / (MODEL // 2)))
        row = lax.broadcasted_iota(jnp.int32, (FINE, MODEL // 2), 0)
        angle = (FINE - 1 - row).astype(F32) * freq
        fine[0] = jnp.sin(angle)
        fine[1] = jnp.cos(angle)
        n = 3 * SEG // FINE
        for part in range(n // 16):
            row = lax.broadcasted_iota(jnp.int32, (16, MODEL // 2), 0) + part * 16
            angle = (FINE * (n - 1 - row)).astype(F32) * freq[:16]
            coarse[0, part * 16 : part * 16 + 16, :] = jnp.sin(angle)
            coarse[1, part * 16 : part * 16 + 16, :] = jnp.cos(angle)

    def rel_rows(c):
        sa, ca = coarse[0, c * 8 : c * 8 + 8, :], coarse[1, c * 8 : c * 8 + 8, :]
        sf, cf = fine[0], fine[1]
        sines, cosines = [], []
        for b in range(8):
            sb, cb = sa[b : b + 1], ca[b : b + 1]
            sines.append((sb * cf + cb * sf).astype(BF16))
            cosines.append((cb * cf - sb * sf).astype(BF16))
        half = MODEL // 2
        total = dot(jnp.concatenate(sines, 0), wp[:half]) + dot(jnp.concatenate(cosines, 0), wp[half:])
        rel[c * 256 : (c + 1) * 256, :] = total.astype(BF16)

    other_slot = jnp.where(front, 3, 0)

    def kv_rows(slot, r):
        return pl.ds(pl.multiple_of(slot * SEG + r * ROWS, ROWS), ROWS)

    def shift_line(r):
        return copy_to(kv.at[kv_rows(3, r)], kv.at[kv_rows(0, r)], (y_s, y_r), r, next_line)

    def shift_line_in(r):
        return copy_to(kv.at[kv_rows(3, r)], kv.at[kv_rows(0, r)], (y_s, y_r), r, prev_line)

    def to_twin(slot, r):
        return copy_to(kv.at[kv_rows(slot, r)], kv.at[kv_rows(1, r)], (d_s, d_r), r, twin)

    def project(r):
        rows = pl.ds(r * ROWS, ROWS)
        mine = g[low, rows, :]
        both = jnp.concatenate([mine, g[1 - low, rows, :]], 0)
        made = dot(both, wkv[...]).astype(BF16)
        kv[kv_rows(2, r), :] = made[:ROWS]
        kv[kv_rows(other_slot, r), :] = made[ROWS:]

        @pl.when(has_next)
        def _():
            shift_line(r).start()

        @pl.when(core == 0)
        def _():
            to_twin(2, r).start()

        @pl.when(jnp.logical_and(core == 1, low == 1))
        def _():
            to_twin(0, r).start()

        q = dot(mine, wq[...]).astype(BF16).astype(F32)
        for h in range(4):
            cols = slice(h * HEAD, (h + 1) * HEAD)
            cq[r * ROWS : (r + 1) * ROWS, cols] = (q[:, cols] + bc[h : h + 1, :]).astype(BF16)
            pq[r * ROWS : (r + 1) * ROWS, cols] = (q[:, cols] + bp[h : h + 1, :]).astype(BF16)

    @pl.when(jnp.logical_and(front, s < 4))
    def _():
        kv[0:SEG, :] = jnp.zeros((SEG, 2 * WIDTH), BF16)

    rel[3 * SEG :, :] = jnp.zeros((ROWS, WIDTH), BF16)

    tables()
    loads[0].wait()
    pl.semaphore_wait(barrier, 8)

    projected = False
    passed, made = 0, 0
    for _, way, p, d in gather_order():
        if way < 2:
            if d > 0:
                came(way, p, d).wait_recv()
            send(way, p, d).start()
            passed += 1
            if passed % 4 == 2 and passed > 4 and made < 6:
                if made == 0:
                    loads[1].wait()
                rel_rows(made)
                made += 1
            continue
        if not projected:
            for load in loads[2:5]:
                load.wait()
            projected = True
        for piece in range(p * ROWS // PIECE, (p + 1) * ROWS // PIECE):
            came(0, piece, REACH[0][piece]).wait_recv()
            came(1, piece, REACH[1][piece]).wait_recv()
        project(p)

    for r in range(CHUNKS):
        @pl.when(has_prev)
        def _():
            shift_line_in(r).wait_recv()

        @pl.when(jnp.logical_and(core == 1, front))
        def _():
            to_twin(0, r).start()

    for r in range(CHUNKS):
        to_twin(0, r).wait_recv()
    for load in loads[5:]:
        load.wait()

    start = jnp.maximum(2 * SEG - SEG * s, 0)
    scale = math.log2(math.e) / math.sqrt(HEAD)

    def attend(r):
        i0 = r * ROWS
        keys = 2 * SEG + ROWS + i0
        span = keys + ROWS
        e0 = SEG - ROWS - i0
        outside = jnp.where(lax.broadcasted_iota(jnp.int32, (1, keys), 1) >= start, 0.0, NEG).astype(F32)
        causal = lax.broadcasted_iota(jnp.int32, (ROWS, ROWS), 1) <= lax.broadcasted_iota(jnp.int32, (ROWS, ROWS), 0)

        def one(h):
            cols = slice(h * HEAD, (h + 1) * HEAD)
            vcols = slice(WIDTH + h * HEAD, WIDTH + (h + 1) * HEAD)
            content = dot_t(cq[i0 : i0 + ROWS, cols], kv[0:keys, cols])
            position = dot_t(pq[i0 : i0 + ROWS, cols], rel[e0 : e0 + span, cols])
            position = pltpu.roll(position, span - (ROWS - 1), 1, stride=1, stride_axis=0)[:, :keys]
            score = content + position + outside
            tail = jnp.where(causal, score[:, keys - ROWS :], NEG)
            score = jnp.concatenate([score[:, : keys - ROWS], tail], 1)
            top = jnp.max(score, axis=1, keepdims=True)
            e = jnp.exp2((score - top) * scale)
            norm = 1.0 / jnp.sum(e, axis=1, keepdims=True)
            att[i0 : i0 + ROWS, cols] = dot((e * norm).astype(BF16), kv[0:keys, vcols]).astype(BF16)

        for h in range(4):
            one(h)

    def opp_right(r):
        return copy_to(opp.at[r, pl.ds(0, HALF)], half_r.at[r], (or_s, or_r), r, to_right)

    def opp_left(r):
        return copy_to(opp.at[r, pl.ds(HALF, HALF)], half_l.at[r], (ol_s, ol_r), r, to_left)

    def fin_right(r, i):
        rows = pl.ds((1 - i) * HALF, HALF)
        return copy_to(near_r.at[r, rows], fin_r.at[r, rows], (fr_s, fr_r), (i, r), to_right)

    def fin_left(r, i):
        rows = pl.ds(i * HALF, HALF)
        return copy_to(near_l.at[r, rows], fin_l.at[r, rows], (fl_s, fl_r), (i, r), to_left)

    def output(r):
        a = att[r * ROWS : (r + 1) * ROWS, :]
        opp[r] = dot(a, wo[across]).astype(BF16)
        opp_right(r).start()
        opp_left(r).start()
        near_r[r] = dot(a, wo[right]).astype(BF16)
        fin_right(r, 0).start()
        near_l[r] = dot(a, wo[left]).astype(BF16)
        fin_left(r, 0).start()
        own[r] = dot(a, wo[t]).astype(BF16)

    def pass_on(r):
        opp_right(r).wait_recv()
        near_r[r, :HALF, :] = (near_r[r, :HALF, :].astype(F32) + half_r[r].astype(F32)).astype(BF16)
        fin_right(r, 1).start()
        opp_left(r).wait_recv()
        near_l[r, HALF:, :] = (near_l[r, HALF:, :].astype(F32) + half_l[r].astype(F32)).astype(BF16)
        fin_left(r, 1).start()

    others = (to_right, to_across, to_left)

    def stats_to(i, r):
        return copy_to(st_out.at[r], st_in.at[i, r], (st_s, st_r), (i, r), others[i])

    def collect(r):
        for i in range(2):
            fin_right(r, i).wait_recv()
            fin_left(r, i).wait_recv()
        rows = pl.ds(r * ROWS, ROWS)
        total = g[low, rows, own_cols].astype(F32) + (
            own[r].astype(F32) + fin_r[r].astype(F32) + fin_l[r].astype(F32)
        )
        y[r] = total
        mean = jnp.sum(total, axis=1, keepdims=True) * (1.0 / WIDTH)
        centred = total - mean
        square = jnp.sum(centred * centred, axis=1, keepdims=True)
        lane = lax.broadcasted_iota(jnp.int32, (ROWS, 128), 1)
        both = jnp.where(lane == 0, mean, jnp.where(lane == 1, square, 0.0))
        st_out[r] = both.T[:8, :]
        for i in range(3):
            stats_to(i, r).start()

    def finish(r):
        for i in range(3):
            stats_to(i, r).wait_recv()
        stack = jnp.concatenate(
            [st_out[r], st_in[0, r], st_in[1, r], st_in[2, r], jnp.zeros((96, 128), F32)], 0
        ).T
        means = [stack[:, 8 * i : 8 * i + 1] for i in range(4)]
        squares = [stack[:, 8 * i + 1 : 8 * i + 2] for i in range(4)]
        mean = (means[0] + means[1] + means[2] + means[3]) * 0.25
        square = squares[0] + squares[1] + squares[2] + squares[3]
        for m in means:
            square = square + WIDTH * ((m - mean) * (m - mean))
        factor = lax.rsqrt(square * (1.0 / MODEL) + 1e-05)
        normed = (y[r] - mean) * factor
        out[r * ROWS : (r + 1) * ROWS, :] = (normed * gain[...] + shift[...]).astype(BF16)

    for r in range(CHUNKS):
        attend(r)
        output(r)
        if r >= 1:
            pass_on(r - 1)
        if r >= 2:
            collect(r - 2)
    pass_on(CHUNKS - 1)
    collect(CHUNKS - 2)
    for r in range(CHUNKS - 1):
        finish(r)
    collect(CHUNKS - 1)
    finish(CHUNKS - 1)

    for way in range(2):
        for p in range(PIECES):
            for d in range(REACH[way][p]):
                send(way, p, d).wait_send()
    for r in range(CHUNKS):
        @pl.when(has_next)
        def _():
            shift_line(r).wait_send()

        to_twin(0, r).wait_send()
        for copy in (opp_right(r), opp_left(r), fin_right(r, 0), fin_left(r, 0), fin_right(r, 1), fin_left(r, 1)):
            copy.wait_send()
        for i in range(3):
            stats_to(i, r).wait_send()


def layer(n_seq, hidden_in, w_query, w_key, w_value, w_pos, w_out, bias_content, bias_pos, norm_gain, norm_bias):
    anywhere = pl.BlockSpec(memory_space=pl.ANY)
    vmem = pl.BlockSpec(memory_space=pltpu.VMEM)
    dma = pltpu.SemaphoreType.DMA
    per_chunk = [dma((CHUNKS,))] * 2
    return pl.pallas_call(
        functools.partial(kernel, n_seq),
        out_shape=jax.ShapeDtypeStruct((SEG, WIDTH), BF16),
        in_specs=[anywhere] * 6 + [vmem] * 4,
        out_specs=vmem,
        scratch_shapes=[
            pltpu.VMEM((2, SEG, MODEL), BF16),
            pltpu.VMEM((MODEL, WIDTH), BF16),
            pltpu.VMEM((MODEL, 2 * WIDTH), BF16),
            pltpu.VMEM((MODEL, WIDTH), BF16),
            pltpu.VMEM((4, WIDTH, WIDTH), BF16),
            pltpu.VMEM((4 * SEG, 2 * WIDTH), BF16),
            pltpu.VMEM((SEG, WIDTH), BF16),
            pltpu.VMEM((SEG, WIDTH), BF16),
            pltpu.VMEM((3 * SEG + ROWS, WIDTH), BF16),
            pltpu.VMEM((2, FINE, MODEL // 2), F32),
            pltpu.VMEM((2, 3 * SEG // FINE, MODEL // 2), F32),
            pltpu.VMEM((SEG, WIDTH), BF16),
            pltpu.VMEM((CHUNKS, ROWS, WIDTH), BF16),
            pltpu.VMEM((CHUNKS, ROWS, WIDTH), BF16),
            pltpu.VMEM((CHUNKS, ROWS, WIDTH), BF16),
            pltpu.VMEM((CHUNKS, ROWS, WIDTH), BF16),
            pltpu.VMEM((CHUNKS, HALF, WIDTH), BF16),
            pltpu.VMEM((CHUNKS, HALF, WIDTH), BF16),
            pltpu.VMEM((CHUNKS, ROWS, WIDTH), BF16),
            pltpu.VMEM((CHUNKS, ROWS, WIDTH), BF16),
            pltpu.VMEM((CHUNKS, ROWS, WIDTH), F32),
            pltpu.VMEM((CHUNKS, 8, 128), F32),
            pltpu.VMEM((3, CHUNKS, 8, 128), F32),
            dma((9,)),
            dma((4, PIECES)), dma((4, PIECES)), dma((4, PIECES)), dma((4, PIECES)),
            *per_chunk, *per_chunk, *per_chunk, *per_chunk,
            dma((2, CHUNKS)), dma((2, CHUNKS)), dma((2, CHUNKS)), dma((2, CHUNKS)),
            dma((3, CHUNKS)), dma((3, CHUNKS)),
        ],
        compiler_params=pltpu.CompilerParams(
            collective_id=0, has_side_effects=True, vmem_limit_bytes=60 * 2**20
        ),
    )(
        hidden_in, w_query, w_key, w_value, w_pos, w_out, bias_content, bias_pos,
        norm_gain.reshape(1, WIDTH), norm_bias.reshape(1, WIDTH),
    )


def solution(mesh):
    in_specs = (
        P("seq", "tp"),
        P(None, "tp"),
        P(None, "tp"),
        P(None, "tp"),
        P(None, "tp"),
        P("tp", None),
        P("tp", None),
        P("tp", None),
        P("tp"),
        P("tp"),
    )
    return jax.shard_map(
        functools.partial(layer, mesh.shape["seq"]),
        mesh=mesh,
        in_specs=in_specs,
        out_specs=P("seq", "tp"),
        check_vma=False,
    )
```

```python
import functools
import math

import jax
import jax.numpy as jnp
from jax import lax
from jax.experimental import pallas as pl
from jax.experimental.pallas import tpu as pltpu
from jax.sharding import PartitionSpec as P

MESH = pl.DeviceIdType.MESH
F32 = jnp.float32
BF16 = jnp.bfloat16
SEG = 512
ROWS = 128
CHUNKS = SEG // ROWS
HALF = ROWS // 2
PIECE = 64
PIECES = SEG // PIECE
WIDTH = 512
MODEL = 2048
HEAD = 128
FINE = 32
NEG = -1e30


def dot(a, b):
    return jnp.dot(a, b, preferred_element_type=F32)


def dot_t(a, b):
    return lax.dot_general(a, b, (((1,), (1,)), ((), ())), preferred_element_type=F32)


def copy_to(src, dst, sems, at, device):
    return pltpu.make_async_remote_copy(
        src_ref=src,
        dst_ref=dst,
        send_sem=sems[0].at[at],
        recv_sem=sems[1].at[at],
        device_id=device,
        device_id_type=MESH,
    )


def gather_order(slot=1.4, latency=3.6, weight=0.5):
    events = []
    done = [0.0] * PIECES
    for way, reach in enumerate(REACH):
        clock, ends = 0.0, {}
        left = [(p, d) for p in range(PIECES) for d in range(reach[p])]
        while left:
            ready = {(p, d): 0.0 if d == 0 else ends[p, d - 1] + latency for p, d in left if d == 0 or (p, d - 1) in ends}
            clock = max(clock, min(ready.values()))
            pick = min((x for x in ready if ready[x] <= clock + 1e-9), key=lambda x: (weight * x[0] - reach[x[0]] + x[1], x[0]))
            left.remove(pick)
            events.append((clock, way, *pick))
            clock += slot
            ends[pick] = clock
        for p in range(PIECES):
            done[p] = max(done[p], ends[p, reach[p] - 1] + latency)
    for c in range(CHUNKS):
        per = ROWS // PIECE
        events.append((max(done[c * per : (c + 1) * per]), 2, c, 0))
    return sorted(events)


REACH = ([4 if p % 2 == 0 else 3 for p in range(PIECES)], [3 if p % 2 == 0 else 4 for p in range(PIECES)])


def kernel(
    n_seq,
    hid, wq_in, wk_in, wv_in, wp_in, wo_in, bc, bp, gain, shift, out,
    g, wq, wkv, wp, wo, kv, cq, pq, rel, fine, coarse, att,
    opp, near_r, near_l, own, half_r, half_l, fin_r, fin_l, y, st_out, st_in,
    loc, up_s, up_r, dn_s, dn_r, y_s, y_r, d_s, d_r,
    or_s, or_r, ol_s, ol_r, fr_s, fr_r, fl_s, fl_r, st_s, st_r,
):
    s = lax.axis_index("seq")
    t = lax.axis_index("tp")
    core = lax.rem(s, 2)
    low = lax.rem(s // 2, 2)
    z = 2 * t + low
    right, left, across = lax.rem(t + 1, 4), lax.rem(t + 3, 4), lax.rem(t + 2, 4)
    mate = s + 2 - 4 * low
    up = (mate, lax.rem(t + low, 4))
    down = (mate, lax.rem(t + 3 + low, 4))
    twin = (s + 1 - 2 * core, t)
    to_right, to_left, to_across = (s, right), (s, left), (s, across)
    front = low == 0
    has_next = jnp.logical_and(front, s + 4 < n_seq)
    has_prev = jnp.logical_and(front, s >= 4)
    next_line = (lax.rem(s + 4, n_seq), t)
    prev_line = (lax.rem(s + n_seq - 4, n_seq), t)

    barrier = pltpu.get_barrier_semaphore()
    for device in (up, down, twin, to_right, to_left, to_across, next_line, prev_line):
        pl.semaphore_signal(barrier, inc=1, device_id=device, device_id_type=MESH)

    own_cols = pl.ds(pl.multiple_of(t * WIDTH, WIDTH), WIDTH)
    loads = [
        pltpu.make_async_copy(hid, g.at[low, :, own_cols], loc.at[0]),
        pltpu.make_async_copy(wp_in, wp, loc.at[1]),
        pltpu.make_async_copy(wk_in, wkv.at[:, pl.ds(0, WIDTH)], loc.at[2]),
        pltpu.make_async_copy(wv_in, wkv.at[:, pl.ds(WIDTH, WIDTH)], loc.at[3]),
        pltpu.make_async_copy(wq_in, wq, loc.at[4]),
    ]
    for c in range(4):
        loads.append(pltpu.make_async_copy(wo_in.at[:, pl.ds(c * WIDTH, WIDTH)], wo.at[c], loc.at[5 + c]))
    for load in loads:
        load.start()

    def block(z_from, p):
        cols = pl.ds(pl.multiple_of((z_from // 2) * WIDTH, WIDTH), WIDTH)
        return g.at[lax.rem(z_from, 2), pl.ds(p * PIECE, PIECE), cols]

    def send(way, p, d):
        ref = block(lax.rem(z + d, 8) if way else lax.rem(z + 8 - d, 8), p)
        return copy_to(ref, ref, (dn_s, dn_r) if way else (up_s, up_r), (d, p), down if way else up)

    def came(way, p, d):
        ref = block(lax.rem(z + d, 8) if way else lax.rem(z + 8 - d, 8), p)
        return copy_to(ref, ref, (dn_s, dn_r) if way else (up_s, up_r), (d - 1, p), up if way else down)

    def tables():
        k = lax.broadcasted_iota(jnp.int32, (FINE, MODEL // 2), 1).astype(F32)
        freq = jnp.exp(k * (-math.log(10000.0) / (MODEL // 2)))
        row = lax.broadcasted_iota(jnp.int32, (FINE, MODEL // 2), 0)
        angle = (FINE - 1 - row).astype(F32) * freq
        fine[0] = jnp.sin(angle)
        fine[1] = jnp.cos(angle)
        n = 3 * SEG // FINE
        for part in range(n // 16):
            row = lax.broadcasted_iota(jnp.int32, (16, MODEL // 2), 0) + part * 16
            angle = (FINE * (n - 1 - row)).astype(F32) * freq[:16]
            coarse[0, part * 16 : part * 16 + 16, :] = jnp.sin(angle)
            coarse[1, part * 16 : part * 16 + 16, :] = jnp.cos(angle)

    def rel_rows(c):
        sa, ca = coarse[0, c * 8 : c * 8 + 8, :], coarse[1, c * 8 : c * 8 + 8, :]
        sf, cf = fine[0], fine[1]
        sines, cosines = [], []
        for b in range(8):
            sb, cb = sa[b : b + 1], ca[b : b + 1]
            sines.append((sb * cf + cb * sf).astype(BF16))
            cosines.append((cb * cf - sb * sf).astype(BF16))
        half = MODEL // 2
        total = dot(jnp.concatenate(sines, 0), wp[:half]) + dot(jnp.concatenate(cosines, 0), wp[half:])
        rel[c * 256 : (c + 1) * 256, :] = total.astype(BF16)

    other_slot = jnp.where(front, 3, 0)

    def kv_rows(slot, r):
        return pl.ds(pl.multiple_of(slot * SEG + r * ROWS, ROWS), ROWS)

    def shift_line(r):
        return copy_to(kv.at[kv_rows(3, r)], kv.at[kv_rows(0, r)], (y_s, y_r), r, next_line)

    def shift_line_in(r):
        return copy_to(kv.at[kv_rows(3, r)], kv.at[kv_rows(0, r)], (y_s, y_r), r, prev_line)

    def to_twin(slot, r):
        return copy_to(kv.at[kv_rows(slot, r)], kv.at[kv_rows(1, r)], (d_s, d_r), r, twin)

    def project(r):
        rows = pl.ds(r * ROWS, ROWS)
        mine = g[low, rows, :]
        both = jnp.concatenate([mine, g[1 - low, rows, :]], 0)
        made = dot(both, wkv[...]).astype(BF16)
        kv[kv_rows(2, r), :] = made[:ROWS]
        kv[kv_rows(other_slot, r), :] = made[ROWS:]

        @pl.when(has_next)
        def _():
            shift_line(r).start()

        @pl.when(core == 0)
        def _():
            to_twin(2, r).start()

        @pl.when(jnp.logical_and(core == 1, low == 1))
        def _():
            to_twin(0, r).start()

        q = dot(mine, wq[...]).astype(BF16).astype(F32)
        for h in range(4):
            cols = slice(h * HEAD, (h + 1) * HEAD)
            cq[r * ROWS : (r + 1) * ROWS, cols] = (q[:, cols] + bc[h : h + 1, :]).astype(BF16)
            pq[r * ROWS : (r + 1) * ROWS, cols] = (q[:, cols] + bp[h : h + 1, :]).astype(BF16)

    @pl.when(jnp.logical_and(front, s < 4))
    def _():
        kv[0:SEG, :] = jnp.zeros((SEG, 2 * WIDTH), BF16)

    rel[3 * SEG :, :] = jnp.zeros((ROWS, WIDTH), BF16)

    loads[0].wait()
    pl.semaphore_wait(barrier, 8)

    projected = False
    passed, made = 0, 0
    for _, way, p, d in gather_order():
        if way < 2:
            if d > 0:
                came(way, p, d).wait_recv()
            send(way, p, d).start()
            passed += 1
            if passed == 6:
                tables()
            if passed % 4 == 2 and passed > 8 and made < 6:
                if made == 0:
                    loads[1].wait()
                rel_rows(made)
                made += 1
            continue
        if not projected:
            for load in loads[2:5]:
                load.wait()
            projected = True
        for piece in range(p * ROWS // PIECE, (p + 1) * ROWS // PIECE):
            came(0, piece, REACH[0][piece]).wait_recv()
            came(1, piece, REACH[1][piece]).wait_recv()
        project(p)

    for r in range(CHUNKS):
        @pl.when(has_prev)
        def _():
            shift_line_in(r).wait_recv()

        @pl.when(jnp.logical_and(core == 1, front))
        def _():
            to_twin(0, r).start()

    for r in range(CHUNKS):
        to_twin(0, r).wait_recv()
    for load in loads[5:]:
        load.wait()

    start = jnp.maximum(2 * SEG - SEG * s, 0)
    scale = math.log2(math.e) / math.sqrt(HEAD)

    def attend(r):
        i0 = r * ROWS
        keys = 2 * SEG + ROWS + i0
        span = keys + ROWS
        e0 = SEG - ROWS - i0
        outside = jnp.where(lax.broadcasted_iota(jnp.int32, (1, keys), 1) >= start, 0.0, NEG).astype(F32)
        causal = lax.broadcasted_iota(jnp.int32, (ROWS, ROWS), 1) <= lax.broadcasted_iota(jnp.int32, (ROWS, ROWS), 0)

        def one(h):
            cols = slice(h * HEAD, (h + 1) * HEAD)
            vcols = slice(WIDTH + h * HEAD, WIDTH + (h + 1) * HEAD)
            content = dot_t(cq[i0 : i0 + ROWS, cols], kv[0:keys, cols])
            position = dot_t(pq[i0 : i0 + ROWS, cols], rel[e0 : e0 + span, cols])
            position = pltpu.roll(position, span - (ROWS - 1), 1, stride=1, stride_axis=0)[:, :keys]
            score = content + position + outside
            tail = jnp.where(causal, score[:, keys - ROWS :], NEG)
            score = jnp.concatenate([score[:, : keys - ROWS], tail], 1)
            top = jnp.max(score, axis=1, keepdims=True)
            e = jnp.exp2((score - top) * scale)
            norm = 1.0 / jnp.sum(e, axis=1, keepdims=True)
            att[i0 : i0 + ROWS, cols] = dot((e * norm).astype(BF16), kv[0:keys, vcols]).astype(BF16)

        for h in range(4):
            one(h)

    def opp_right(r):
        return copy_to(opp.at[r, pl.ds(0, HALF)], half_r.at[r], (or_s, or_r), r, to_right)

    def opp_left(r):
        return copy_to(opp.at[r, pl.ds(HALF, HALF)], half_l.at[r], (ol_s, ol_r), r, to_left)

    def fin_right(r, i):
        rows = pl.ds((1 - i) * HALF, HALF)
        return copy_to(near_r.at[r, rows], fin_r.at[r, rows], (fr_s, fr_r), (i, r), to_right)

    def fin_left(r, i):
        rows = pl.ds(i * HALF, HALF)
        return copy_to(near_l.at[r, rows], fin_l.at[r, rows], (fl_s, fl_r), (i, r), to_left)

    def output(r):
        a = att[r * ROWS : (r + 1) * ROWS, :]
        opp[r] = dot(a, wo[across]).astype(BF16)
        opp_right(r).start()
        opp_left(r).start()
        near_r[r] = dot(a, wo[right]).astype(BF16)
        fin_right(r, 0).start()
        near_l[r] = dot(a, wo[left]).astype(BF16)
        fin_left(r, 0).start()
        own[r] = dot(a, wo[t]).astype(BF16)

    def pass_on(r):
        opp_right(r).wait_recv()
        near_r[r, :HALF, :] = (near_r[r, :HALF, :].astype(F32) + half_r[r].astype(F32)).astype(BF16)
        fin_right(r, 1).start()
        opp_left(r).wait_recv()
        near_l[r, HALF:, :] = (near_l[r, HALF:, :].astype(F32) + half_l[r].astype(F32)).astype(BF16)
        fin_left(r, 1).start()

    others = (to_right, to_across, to_left)

    def stats_to(i, r):
        return copy_to(st_out.at[r], st_in.at[i, r], (st_s, st_r), (i, r), others[i])

    def collect(r):
        for i in range(2):
            fin_right(r, i).wait_recv()
            fin_left(r, i).wait_recv()
        rows = pl.ds(r * ROWS, ROWS)
        total = g[low, rows, own_cols].astype(F32) + (
            own[r].astype(F32) + fin_r[r].astype(F32) + fin_l[r].astype(F32)
        )
        y[r] = total
        mean = jnp.sum(total, axis=1, keepdims=True) * (1.0 / WIDTH)
        centred = total - mean
        square = jnp.sum(centred * centred, axis=1, keepdims=True)
        lane = lax.broadcasted_iota(jnp.int32, (ROWS, 128), 1)
        both = jnp.where(lane == 0, mean, jnp.where(lane == 1, square, 0.0))
        st_out[r] = both.T[:8, :]
        for i in range(3):
            stats_to(i, r).start()

    def finish(r):
        for i in range(3):
            stats_to(i, r).wait_recv()
        stack = jnp.concatenate(
            [st_out[r], st_in[0, r], st_in[1, r], st_in[2, r], jnp.zeros((96, 128), F32)], 0
        ).T
        means = [stack[:, 8 * i : 8 * i + 1] for i in range(4)]
        squares = [stack[:, 8 * i + 1 : 8 * i + 2] for i in range(4)]
        mean = (means[0] + means[1] + means[2] + means[3]) * 0.25
        square = squares[0] + squares[1] + squares[2] + squares[3]
        for m in means:
            square = square + WIDTH * ((m - mean) * (m - mean))
        factor = lax.rsqrt(square * (1.0 / MODEL) + 1e-05)
        normed = (y[r] - mean) * factor
        out[r * ROWS : (r + 1) * ROWS, :] = (normed * gain[...] + shift[...]).astype(BF16)

    for r in range(CHUNKS):
        attend(r)
        output(r)
        if r >= 1:
            pass_on(r - 1)
        if r >= 2:
            collect(r - 2)
    pass_on(CHUNKS - 1)
    collect(CHUNKS - 2)
    for r in range(CHUNKS - 1):
        finish(r)
    collect(CHUNKS - 1)
    finish(CHUNKS - 1)

    for way in range(2):
        for p in range(PIECES):
            for d in range(REACH[way][p]):
                send(way, p, d).wait_send()
    for r in range(CHUNKS):
        @pl.when(has_next)
        def _():
            shift_line(r).wait_send()

        to_twin(0, r).wait_send()
        for copy in (opp_right(r), opp_left(r), fin_right(r, 0), fin_left(r, 0), fin_right(r, 1), fin_left(r, 1)):
            copy.wait_send()
        for i in range(3):
            stats_to(i, r).wait_send()


def layer(n_seq, hidden_in, w_query, w_key, w_value, w_pos, w_out, bias_content, bias_pos, norm_gain, norm_bias):
    anywhere = pl.BlockSpec(memory_space=pl.ANY)
    vmem = pl.BlockSpec(memory_space=pltpu.VMEM)
    dma = pltpu.SemaphoreType.DMA
    per_chunk = [dma((CHUNKS,))] * 2
    return pl.pallas_call(
        functools.partial(kernel, n_seq),
        out_shape=pltpu.VMEM((SEG, WIDTH), BF16),
        in_specs=[anywhere] * 6 + [vmem] * 4,
        out_specs=vmem,
        scratch_shapes=[
            pltpu.VMEM((2, SEG, MODEL), BF16),
            pltpu.VMEM((MODEL, WIDTH), BF16),
            pltpu.VMEM((MODEL, 2 * WIDTH), BF16),
            pltpu.VMEM((MODEL, WIDTH), BF16),
            pltpu.VMEM((4, WIDTH, WIDTH), BF16),
            pltpu.VMEM((4 * SEG, 2 * WIDTH), BF16),
            pltpu.VMEM((SEG, WIDTH), BF16),
            pltpu.VMEM((SEG, WIDTH), BF16),
            pltpu.VMEM((3 * SEG + ROWS, WIDTH), BF16),
            pltpu.VMEM((2, FINE, MODEL // 2), F32),
            pltpu.VMEM((2, 3 * SEG // FINE, MODEL // 2), F32),
            pltpu.VMEM((SEG, WIDTH), BF16),
            pltpu.VMEM((CHUNKS, ROWS, WIDTH), BF16),
            pltpu.VMEM((CHUNKS, ROWS, WIDTH), BF16),
            pltpu.VMEM((CHUNKS, ROWS, WIDTH), BF16),
            pltpu.VMEM((CHUNKS, ROWS, WIDTH), BF16),
            pltpu.VMEM((CHUNKS, HALF, WIDTH), BF16),
            pltpu.VMEM((CHUNKS, HALF, WIDTH), BF16),
            pltpu.VMEM((CHUNKS, ROWS, WIDTH), BF16),
            pltpu.VMEM((CHUNKS, ROWS, WIDTH), BF16),
            pltpu.VMEM((CHUNKS, ROWS, WIDTH), F32),
            pltpu.VMEM((CHUNKS, 8, 128), F32),
            pltpu.VMEM((3, CHUNKS, 8, 128), F32),
            dma((9,)),
            dma((4, PIECES)), dma((4, PIECES)), dma((4, PIECES)), dma((4, PIECES)),
            *per_chunk, *per_chunk, *per_chunk, *per_chunk,
            dma((2, CHUNKS)), dma((2, CHUNKS)), dma((2, CHUNKS)), dma((2, CHUNKS)),
            dma((3, CHUNKS)), dma((3, CHUNKS)),
        ],
        compiler_params=pltpu.CompilerParams(
            collective_id=0, has_side_effects=True, vmem_limit_bytes=66_200_000
        ),
    )(
        hidden_in, w_query, w_key, w_value, w_pos, w_out, bias_content, bias_pos,
        norm_gain.reshape(1, WIDTH), norm_bias.reshape(1, WIDTH),
    )


def solution(mesh):
    in_specs = (
        P("seq", "tp"),
        P(None, "tp"),
        P(None, "tp"),
        P(None, "tp"),
        P(None, "tp"),
        P("tp", None),
        P("tp", None),
        P("tp", None),
        P("tp"),
        P("tp"),
    )
    return jax.shard_map(
        functools.partial(layer, mesh.shape["seq"]),
        mesh=mesh,
        in_specs=in_specs,
        out_specs=P("seq", "tp"),
        check_vma=False,
    )
```

```python
import functools
import math

import jax
import jax.numpy as jnp
from jax import lax
from jax.experimental import pallas as pl
from jax.experimental.pallas import tpu as pltpu
from jax.sharding import PartitionSpec as P

MESH = pl.DeviceIdType.MESH
F32 = jnp.float32
BF16 = jnp.bfloat16
SEG = 512
ROWS = 128
CHUNKS = SEG // ROWS
HALF = ROWS // 2
PIECE = 64
PIECES = SEG // PIECE
WIDTH = 512
MODEL = 2048
HEAD = 128
FINE = 32
NEG = -1e30


def dot(a, b):
    return jnp.dot(a, b, preferred_element_type=F32)


def dot_t(a, b):
    return lax.dot_general(a, b, (((1,), (1,)), ((), ())), preferred_element_type=F32)


def copy_to(src, dst, sems, at, device):
    return pltpu.make_async_remote_copy(
        src_ref=src,
        dst_ref=dst,
        send_sem=sems[0].at[at],
        recv_sem=sems[1].at[at],
        device_id=device,
        device_id_type=MESH,
    )


def gather_order(slot=1.4, latency=3.0, weight=0.34):
    events = []
    done = [0.0] * PIECES
    for way, reach in enumerate(REACH):
        clock, ends = 0.0, {}
        left = [(p, d) for p in range(PIECES) for d in range(reach[p])]
        while left:
            ready = {(p, d): 0.0 if d == 0 else ends[p, d - 1] + latency for p, d in left if d == 0 or (p, d - 1) in ends}
            clock = max(clock, min(ready.values()))
            pick = min((x for x in ready if ready[x] <= clock + 1e-9), key=lambda x: (weight * x[0] - reach[x[0]] + x[1], x[0]))
            left.remove(pick)
            events.append((clock, way, *pick))
            clock += slot
            ends[pick] = clock
        for p in range(PIECES):
            done[p] = max(done[p], ends[p, reach[p] - 1] + latency)
    for c in range(CHUNKS):
        per = ROWS // PIECE
        events.append((max(done[c * per : (c + 1) * per]), 2, c, 0))
    return sorted(events)


REACH = ([4 if p % 2 == 0 else 3 for p in range(PIECES)], [3 if p % 2 == 0 else 4 for p in range(PIECES)])


def kernel(
    n_seq,
    hid, wq_in, wk_in, wv_in, wp_in, wo_in, bc, bp, gain, shift, out,
    g, wq, wkv, wp, wo, kv, cq, pq, rel, fine, coarse, att,
    opp, near_r, near_l, own, half_r, half_l, fin_r, fin_l, y, st_out, st_in,
    loc, up_s, up_r, dn_s, dn_r, y_s, y_r, d_s, d_r,
    or_s, or_r, ol_s, ol_r, fr_s, fr_r, fl_s, fl_r, st_s, st_r,
):
    s = lax.axis_index("seq")
    t = lax.axis_index("tp")
    core = lax.rem(s, 2)
    low = lax.rem(s // 2, 2)
    z = 2 * t + low
    right, left, across = lax.rem(t + 1, 4), lax.rem(t + 3, 4), lax.rem(t + 2, 4)
    mate = s + 2 - 4 * low
    up = (mate, lax.rem(t + low, 4))
    down = (mate, lax.rem(t + 3 + low, 4))
    twin = (s + 1 - 2 * core, t)
    to_right, to_left, to_across = (s, right), (s, left), (s, across)
    front = low == 0
    has_next = jnp.logical_and(front, s + 4 < n_seq)
    has_prev = jnp.logical_and(front, s >= 4)
    next_line = (lax.rem(s + 4, n_seq), t)
    prev_line = (lax.rem(s + n_seq - 4, n_seq), t)

    barrier = pltpu.get_barrier_semaphore()
    for device in (up, down, twin, to_right, to_left, to_across, next_line, prev_line):
        pl.semaphore_signal(barrier, inc=1, device_id=device, device_id_type=MESH)

    own_cols = pl.ds(pl.multiple_of(t * WIDTH, WIDTH), WIDTH)
    loads = [
        pltpu.make_async_copy(hid, g.at[low, :, own_cols], loc.at[0]),
        pltpu.make_async_copy(wp_in, wp, loc.at[1]),
        pltpu.make_async_copy(wk_in, wkv.at[:, pl.ds(0, WIDTH)], loc.at[2]),
        pltpu.make_async_copy(wv_in, wkv.at[:, pl.ds(WIDTH, WIDTH)], loc.at[3]),
        pltpu.make_async_copy(wq_in, wq, loc.at[4]),
    ]
    for c in range(4):
        loads.append(pltpu.make_async_copy(wo_in.at[:, pl.ds(c * WIDTH, WIDTH)], wo.at[c], loc.at[5 + c]))
    for load in loads:
        load.start()

    def block(z_from, p):
        cols = pl.ds(pl.multiple_of((z_from // 2) * WIDTH, WIDTH), WIDTH)
        return g.at[lax.rem(z_from, 2), pl.ds(p * PIECE, PIECE), cols]

    def send(way, p, d):
        ref = block(lax.rem(z + d, 8) if way else lax.rem(z + 8 - d, 8), p)
        return copy_to(ref, ref, (dn_s, dn_r) if way else (up_s, up_r), (d, p), down if way else up)

    def came(way, p, d):
        ref = block(lax.rem(z + d, 8) if way else lax.rem(z + 8 - d, 8), p)
        return copy_to(ref, ref, (dn_s, dn_r) if way else (up_s, up_r), (d - 1, p), up if way else down)

    def tables():
        k = lax.broadcasted_iota(jnp.int32, (FINE, MODEL // 2), 1).astype(F32)
        freq = jnp.exp(k * (-math.log(10000.0) / (MODEL // 2)))
        row = lax.broadcasted_iota(jnp.int32, (FINE, MODEL // 2), 0)
        angle = (FINE - 1 - row).astype(F32) * freq
        fine[0] = jnp.sin(angle)
        fine[1] = jnp.cos(angle)
        n = 3 * SEG // FINE
        for part in range(n // 16):
            row = lax.broadcasted_iota(jnp.int32, (16, MODEL // 2), 0) + part * 16
            angle = (FINE * (n - 1 - row)).astype(F32) * freq[:16]
            coarse[0, part * 16 : part * 16 + 16, :] = jnp.sin(angle)
            coarse[1, part * 16 : part * 16 + 16, :] = jnp.cos(angle)

    def rel_rows(c):
        sa, ca = coarse[0, c * 8 : c * 8 + 8, :], coarse[1, c * 8 : c * 8 + 8, :]
        sf, cf = fine[0], fine[1]
        sines, cosines = [], []
        for b in range(8):
            sb, cb = sa[b : b + 1], ca[b : b + 1]
            sines.append((sb * cf + cb * sf).astype(BF16))
            cosines.append((cb * cf - sb * sf).astype(BF16))
        half = MODEL // 2
        total = dot(jnp.concatenate(sines, 0), wp[:half]) + dot(jnp.concatenate(cosines, 0), wp[half:])
        rel[c * 256 : (c + 1) * 256, :] = total.astype(BF16)

    other_slot = jnp.where(front, 3, 0)

    def kv_rows(slot, r):
        return pl.ds(pl.multiple_of(slot * SEG + r * ROWS, ROWS), ROWS)

    def shift_line(r):
        return copy_to(kv.at[kv_rows(3, r)], kv.at[kv_rows(0, r)], (y_s, y_r), r, next_line)

    def shift_line_in(r):
        return copy_to(kv.at[kv_rows(3, r)], kv.at[kv_rows(0, r)], (y_s, y_r), r, prev_line)

    def to_twin(slot, r):
        return copy_to(kv.at[kv_rows(slot, r)], kv.at[kv_rows(1, r)], (d_s, d_r), r, twin)

    def project(r):
        rows = pl.ds(r * ROWS, ROWS)
        mine = g[low, rows, :]
        both = jnp.concatenate([mine, g[1 - low, rows, :]], 0)
        made = dot(both, wkv[...]).astype(BF16)
        kv[kv_rows(2, r), :] = made[:ROWS]
        kv[kv_rows(other_slot, r), :] = made[ROWS:]

        @pl.when(has_next)
        def _():
            shift_line(r).start()

        @pl.when(core == 0)
        def _():
            to_twin(2, r).start()

        @pl.when(jnp.logical_and(core == 1, low == 1))
        def _():
            to_twin(0, r).start()

        q = dot(mine, wq[...]).astype(BF16).astype(F32)
        for h in range(4):
            cols = slice(h * HEAD, (h + 1) * HEAD)
            cq[r * ROWS : (r + 1) * ROWS, cols] = (q[:, cols] + bc[h : h + 1, :]).astype(BF16)
            pq[r * ROWS : (r + 1) * ROWS, cols] = (q[:, cols] + bp[h : h + 1, :]).astype(BF16)

    @pl.when(jnp.logical_and(front, s < 4))
    def _():
        kv[0:SEG, :] = jnp.zeros((SEG, 2 * WIDTH), BF16)

    rel[3 * SEG :, :] = jnp.zeros((ROWS, WIDTH), BF16)

    loads[0].wait()
    pl.semaphore_wait(barrier, 8)

    projected = False
    passed, made = 0, 0
    for _, way, p, d in gather_order():
        if way < 2:
            if d > 0:
                came(way, p, d).wait_recv()
            send(way, p, d).start()
            passed += 1
            if passed == 6:
                tables()
            if passed % 4 == 2 and passed > 8 and made < 6:
                if made == 0:
                    loads[1].wait()
                rel_rows(made)
                made += 1
            continue
        if not projected:
            for load in loads[2:5]:
                load.wait()
            projected = True
        for piece in range(p * ROWS // PIECE, (p + 1) * ROWS // PIECE):
            came(0, piece, REACH[0][piece]).wait_recv()
            came(1, piece, REACH[1][piece]).wait_recv()
        project(p)

    for r in range(CHUNKS):
        @pl.when(has_prev)
        def _():
            shift_line_in(r).wait_recv()

        @pl.when(jnp.logical_and(core == 1, front))
        def _():
            to_twin(0, r).start()

    for r in range(CHUNKS):
        to_twin(0, r).wait_recv()
    for load in loads[5:]:
        load.wait()

    start = jnp.maximum(2 * SEG - SEG * s, 0)
    scale = math.log2(math.e) / math.sqrt(HEAD)

    def attend(r):
        i0 = r * ROWS
        keys = 2 * SEG + ROWS + i0
        span = keys + ROWS
        e0 = SEG - ROWS - i0
        outside = jnp.where(lax.broadcasted_iota(jnp.int32, (1, keys), 1) >= start, 0.0, NEG).astype(F32)
        causal = lax.broadcasted_iota(jnp.int32, (ROWS, ROWS), 1) <= lax.broadcasted_iota(jnp.int32, (ROWS, ROWS), 0)

        def one(h):
            cols = slice(h * HEAD, (h + 1) * HEAD)
            vcols = slice(WIDTH + h * HEAD, WIDTH + (h + 1) * HEAD)
            content = dot_t(cq[i0 : i0 + ROWS, cols], kv[0:keys, cols])
            position = dot_t(pq[i0 : i0 + ROWS, cols], rel[e0 : e0 + span, cols])
            position = pltpu.roll(position, span - (ROWS - 1), 1, stride=1, stride_axis=0)[:, :keys]
            score = content + position + outside
            tail = jnp.where(causal, score[:, keys - ROWS :], NEG)
            score = jnp.concatenate([score[:, : keys - ROWS], tail], 1)
            top = jnp.max(score, axis=1, keepdims=True)
            e = jnp.exp2((score - top) * scale)
            norm = 1.0 / jnp.sum(e, axis=1, keepdims=True)
            att[i0 : i0 + ROWS, cols] = dot((e * norm).astype(BF16), kv[0:keys, vcols]).astype(BF16)

        for h in range(4):
            one(h)

    def opp_right(r):
        return copy_to(opp.at[r, pl.ds(0, HALF)], half_r.at[r], (or_s, or_r), r, to_right)

    def opp_left(r):
        return copy_to(opp.at[r, pl.ds(HALF, HALF)], half_l.at[r], (ol_s, ol_r), r, to_left)

    def fin_right(r, i):
        rows = pl.ds((1 - i) * HALF, HALF)
        return copy_to(near_r.at[r, rows], fin_r.at[r, rows], (fr_s, fr_r), (i, r), to_right)

    def fin_left(r, i):
        rows = pl.ds(i * HALF, HALF)
        return copy_to(near_l.at[r, rows], fin_l.at[r, rows], (fl_s, fl_r), (i, r), to_left)

    def output(r):
        a = att[r * ROWS : (r + 1) * ROWS, :]
        opp[r] = dot(a, wo[across]).astype(BF16)
        opp_right(r).start()
        opp_left(r).start()
        near_r[r] = dot(a, wo[right]).astype(BF16)
        fin_right(r, 0).start()
        near_l[r] = dot(a, wo[left]).astype(BF16)
        fin_left(r, 0).start()
        own[r] = dot(a, wo[t]).astype(BF16)

    def pass_on(r):
        opp_right(r).wait_recv()
        near_r[r, :HALF, :] = (near_r[r, :HALF, :].astype(F32) + half_r[r].astype(F32)).astype(BF16)
        fin_right(r, 1).start()
        opp_left(r).wait_recv()
        near_l[r, HALF:, :] = (near_l[r, HALF:, :].astype(F32) + half_l[r].astype(F32)).astype(BF16)
        fin_left(r, 1).start()

    others = (to_right, to_across, to_left)

    def stats_to(i, r):
        return copy_to(st_out.at[r], st_in.at[i, r], (st_s, st_r), (i, r), others[i])

    def collect(r):
        for i in range(2):
            fin_right(r, i).wait_recv()
            fin_left(r, i).wait_recv()
        rows = pl.ds(r * ROWS, ROWS)
        total = g[low, rows, own_cols].astype(F32) + (
            own[r].astype(F32) + fin_r[r].astype(F32) + fin_l[r].astype(F32)
        )
        y[r] = total
        mean = jnp.sum(total, axis=1, keepdims=True) * (1.0 / WIDTH)
        centred = total - mean
        square = jnp.sum(centred * centred, axis=1, keepdims=True)
        lane = lax.broadcasted_iota(jnp.int32, (ROWS, 128), 1)
        both = jnp.where(lane == 0, mean, jnp.where(lane == 1, square, 0.0))
        st_out[r] = both.T[:8, :]
        for i in range(3):
            stats_to(i, r).start()

    def finish(r):
        for i in range(3):
            stats_to(i, r).wait_recv()
        stack = jnp.concatenate(
            [st_out[r], st_in[0, r], st_in[1, r], st_in[2, r], jnp.zeros((96, 128), F32)], 0
        ).T
        means = [stack[:, 8 * i : 8 * i + 1] for i in range(4)]
        squares = [stack[:, 8 * i + 1 : 8 * i + 2] for i in range(4)]
        mean = (means[0] + means[1] + means[2] + means[3]) * 0.25
        square = squares[0] + squares[1] + squares[2] + squares[3]
        for m in means:
            square = square + WIDTH * ((m - mean) * (m - mean))
        factor = lax.rsqrt(square * (1.0 / MODEL) + 1e-05)
        normed = (y[r] - mean) * factor
        out[r * ROWS : (r + 1) * ROWS, :] = (normed * gain[...] + shift[...]).astype(BF16)

    for r in range(CHUNKS):
        attend(r)
        output(r)
        if r >= 1:
            pass_on(r - 1)
    pass_on(CHUNKS - 1)
    for r in range(CHUNKS):
        collect(r)
        if 1 <= r < CHUNKS - 1:
            finish(r - 1)
    finish(CHUNKS - 2)
    finish(CHUNKS - 1)

    for way in range(2):
        for p in range(PIECES):
            for d in range(REACH[way][p]):
                send(way, p, d).wait_send()
    for r in range(CHUNKS):
        @pl.when(has_next)
        def _():
            shift_line(r).wait_send()

        to_twin(0, r).wait_send()
        for copy in (opp_right(r), opp_left(r), fin_right(r, 0), fin_left(r, 0), fin_right(r, 1), fin_left(r, 1)):
            copy.wait_send()
        for i in range(3):
            stats_to(i, r).wait_send()


def layer(n_seq, hidden_in, w_query, w_key, w_value, w_pos, w_out, bias_content, bias_pos, norm_gain, norm_bias):
    anywhere = pl.BlockSpec(memory_space=pl.ANY)
    vmem = pl.BlockSpec(memory_space=pltpu.VMEM)
    dma = pltpu.SemaphoreType.DMA
    per_chunk = [dma((CHUNKS,))] * 2
    return pl.pallas_call(
        functools.partial(kernel, n_seq),
        out_shape=pltpu.VMEM((SEG, WIDTH), BF16),
        in_specs=[anywhere] * 6 + [vmem] * 4,
        out_specs=vmem,
        scratch_shapes=[
            pltpu.VMEM((2, SEG, MODEL), BF16),
            pltpu.VMEM((MODEL, WIDTH), BF16),
            pltpu.VMEM((MODEL, 2 * WIDTH), BF16),
            pltpu.VMEM((MODEL, WIDTH), BF16),
            pltpu.VMEM((4, WIDTH, WIDTH), BF16),
            pltpu.VMEM((4 * SEG, 2 * WIDTH), BF16),
            pltpu.VMEM((SEG, WIDTH), BF16),
            pltpu.VMEM((SEG, WIDTH), BF16),
            pltpu.VMEM((3 * SEG + ROWS, WIDTH), BF16),
            pltpu.VMEM((2, FINE, MODEL // 2), F32),
            pltpu.VMEM((2, 3 * SEG // FINE, MODEL // 2), F32),
            pltpu.VMEM((SEG, WIDTH), BF16),
            pltpu.VMEM((CHUNKS, ROWS, WIDTH), BF16),
            pltpu.VMEM((CHUNKS, ROWS, WIDTH), BF16),
            pltpu.VMEM((CHUNKS, ROWS, WIDTH), BF16),
            pltpu.VMEM((CHUNKS, ROWS, WIDTH), BF16),
            pltpu.VMEM((CHUNKS, HALF, WIDTH), BF16),
            pltpu.VMEM((CHUNKS, HALF, WIDTH), BF16),
            pltpu.VMEM((CHUNKS, ROWS, WIDTH), BF16),
            pltpu.VMEM((CHUNKS, ROWS, WIDTH), BF16),
            pltpu.VMEM((CHUNKS, ROWS, WIDTH), F32),
            pltpu.VMEM((CHUNKS, 8, 128), F32),
            pltpu.VMEM((3, CHUNKS, 8, 128), F32),
            dma((9,)),
            dma((4, PIECES)), dma((4, PIECES)), dma((4, PIECES)), dma((4, PIECES)),
            *per_chunk, *per_chunk, *per_chunk, *per_chunk,
            dma((2, CHUNKS)), dma((2, CHUNKS)), dma((2, CHUNKS)), dma((2, CHUNKS)),
            dma((3, CHUNKS)), dma((3, CHUNKS)),
        ],
        compiler_params=pltpu.CompilerParams(
            collective_id=0, has_side_effects=True, vmem_limit_bytes=66_200_000
        ),
    )(
        hidden_in, w_query, w_key, w_value, w_pos, w_out, bias_content, bias_pos,
        norm_gain.reshape(1, WIDTH), norm_bias.reshape(1, WIDTH),
    )


def solution(mesh):
    in_specs = (
        P("seq", "tp"),
        P(None, "tp"),
        P(None, "tp"),
        P(None, "tp"),
        P(None, "tp"),
        P("tp", None),
        P("tp", None),
        P("tp", None),
        P("tp"),
        P("tp"),
    )
    return jax.shard_map(
        functools.partial(layer, mesh.shape["seq"]),
        mesh=mesh,
        in_specs=in_specs,
        out_specs=P("seq", "tp"),
        check_vma=False,
    )
```

```python
import functools
import math

import jax
import jax.numpy as jnp
from jax import lax
from jax.experimental import pallas as pl
from jax.experimental.pallas import tpu as pltpu
from jax.sharding import PartitionSpec as P

MESH = pl.DeviceIdType.MESH
F32 = jnp.float32
BF16 = jnp.bfloat16
SEG = 512
ROWS = 128
CHUNKS = SEG // ROWS
HALF = ROWS // 2
PIECE = 64
PIECES = SEG // PIECE
WIDTH = 512
MODEL = 2048
HEAD = 128
FINE = 32
NEG = -1e30


def dot(a, b):
    return jnp.dot(a, b, preferred_element_type=F32)


def dot_t(a, b):
    return lax.dot_general(a, b, (((1,), (1,)), ((), ())), preferred_element_type=F32)


def copy_to(src, dst, sems, at, device):
    return pltpu.make_async_remote_copy(
        src_ref=src,
        dst_ref=dst,
        send_sem=sems[0].at[at],
        recv_sem=sems[1].at[at],
        device_id=device,
        device_id_type=MESH,
    )


def gather_order(slot=1.4, latency=3.0, weight=0.34):
    events = []
    done = [0.0] * PIECES
    for way, reach in enumerate(REACH):
        clock, ends = 0.0, {}
        left = [(p, d) for p in range(PIECES) for d in range(reach[p])]
        while left:
            ready = {(p, d): 0.0 if d == 0 else ends[p, d - 1] + latency for p, d in left if d == 0 or (p, d - 1) in ends}
            clock = max(clock, min(ready.values()))
            pick = min((x for x in ready if ready[x] <= clock + 1e-9), key=lambda x: (weight * x[0] - reach[x[0]] + x[1], x[0]))
            left.remove(pick)
            events.append((clock, way, *pick))
            clock += slot
            ends[pick] = clock
        for p in range(PIECES):
            done[p] = max(done[p], ends[p, reach[p] - 1] + latency)
    for c in range(CHUNKS):
        per = ROWS // PIECE
        events.append((max(done[c * per : (c + 1) * per]), 2, c, 0))
    return sorted(events)


REACH = ([4 if p % 2 == 0 else 3 for p in range(PIECES)], [3 if p % 2 == 0 else 4 for p in range(PIECES)])


def kernel(
    n_seq,
    hid, wq_in, wk_in, wv_in, wp_in, wo_in, bc, bp, gain, shift, out,
    g, wq, wkv, wp, wo, kv, cq, pq, rel, fine, coarse, att,
    opp, near_r, near_l, own, half_r, half_l, fin_r, fin_l, y, st_out, st_in,
    loc, up_s, up_r, dn_s, dn_r, y_s, y_r, d_s, d_r,
    or_s, or_r, ol_s, ol_r, fr_s, fr_r, fl_s, fl_r, st_s, st_r,
):
    s = lax.axis_index("seq")
    t = lax.axis_index("tp")
    core = lax.rem(s, 2)
    low = lax.rem(s // 2, 2)
    z = 2 * t + low
    right, left, across = lax.rem(t + 1, 4), lax.rem(t + 3, 4), lax.rem(t + 2, 4)
    mate = s + 2 - 4 * low
    up = (mate, lax.rem(t + low, 4))
    down = (mate, lax.rem(t + 3 + low, 4))
    twin = (s + 1 - 2 * core, t)
    to_right, to_left, to_across = (s, right), (s, left), (s, across)
    front = low == 0
    has_next = jnp.logical_and(front, s + 4 < n_seq)
    has_prev = jnp.logical_and(front, s >= 4)
    next_line = (lax.rem(s + 4, n_seq), t)
    prev_line = (lax.rem(s + n_seq - 4, n_seq), t)

    barrier = pltpu.get_barrier_semaphore()
    for device in (up, down, twin, next_line, prev_line):
        pl.semaphore_signal(barrier, inc=1, device_id=device, device_id_type=MESH)

    own_cols = pl.ds(pl.multiple_of(t * WIDTH, WIDTH), WIDTH)
    loads = [
        pltpu.make_async_copy(hid, g.at[low, :, own_cols], loc.at[0]),
        pltpu.make_async_copy(wp_in, wp, loc.at[1]),
        pltpu.make_async_copy(wk_in, wkv.at[:, pl.ds(0, WIDTH)], loc.at[2]),
        pltpu.make_async_copy(wv_in, wkv.at[:, pl.ds(WIDTH, WIDTH)], loc.at[3]),
        pltpu.make_async_copy(wq_in, wq, loc.at[4]),
    ]
    for c in range(4):
        loads.append(pltpu.make_async_copy(wo_in.at[:, pl.ds(c * WIDTH, WIDTH)], wo.at[c], loc.at[5 + c]))
    for load in loads:
        load.start()

    def block(z_from, p):
        cols = pl.ds(pl.multiple_of((z_from // 2) * WIDTH, WIDTH), WIDTH)
        return g.at[lax.rem(z_from, 2), pl.ds(p * PIECE, PIECE), cols]

    def send(way, p, d):
        ref = block(lax.rem(z + d, 8) if way else lax.rem(z + 8 - d, 8), p)
        return copy_to(ref, ref, (dn_s, dn_r) if way else (up_s, up_r), (d, p), down if way else up)

    def came(way, p, d):
        ref = block(lax.rem(z + d, 8) if way else lax.rem(z + 8 - d, 8), p)
        return copy_to(ref, ref, (dn_s, dn_r) if way else (up_s, up_r), (d - 1, p), up if way else down)

    def tables():
        k = lax.broadcasted_iota(jnp.int32, (FINE, MODEL // 2), 1).astype(F32)
        freq = jnp.exp(k * (-math.log(10000.0) / (MODEL // 2)))
        row = lax.broadcasted_iota(jnp.int32, (FINE, MODEL // 2), 0)
        angle = (FINE - 1 - row).astype(F32) * freq
        fine[0] = jnp.sin(angle)
        fine[1] = jnp.cos(angle)
        n = 3 * SEG // FINE
        for part in range(n // 16):
            row = lax.broadcasted_iota(jnp.int32, (16, MODEL // 2), 0) + part * 16
            angle = (FINE * (n - 1 - row)).astype(F32) * freq[:16]
            coarse[0, part * 16 : part * 16 + 16, :] = jnp.sin(angle)
            coarse[1, part * 16 : part * 16 + 16, :] = jnp.cos(angle)

    def rel_rows(c):
        sa, ca = coarse[0, c * 8 : c * 8 + 8, :], coarse[1, c * 8 : c * 8 + 8, :]
        sf, cf = fine[0], fine[1]
        sines, cosines = [], []
        for b in range(8):
            sb, cb = sa[b : b + 1], ca[b : b + 1]
            sines.append((sb * cf + cb * sf).astype(BF16))
            cosines.append((cb * cf - sb * sf).astype(BF16))
        half = MODEL // 2
        total = dot(jnp.concatenate(sines, 0), wp[:half]) + dot(jnp.concatenate(cosines, 0), wp[half:])
        rel[c * 256 : (c + 1) * 256, :] = total.astype(BF16)

    other_slot = jnp.where(front, 3, 0)

    def kv_rows(slot, r):
        return pl.ds(pl.multiple_of(slot * SEG + r * ROWS, ROWS), ROWS)

    def shift_line(r):
        return copy_to(kv.at[kv_rows(3, r)], kv.at[kv_rows(0, r)], (y_s, y_r), r, next_line)

    def shift_line_in(r):
        return copy_to(kv.at[kv_rows(3, r)], kv.at[kv_rows(0, r)], (y_s, y_r), r, prev_line)

    def to_twin(slot, r):
        return copy_to(kv.at[kv_rows(slot, r)], kv.at[kv_rows(1, r)], (d_s, d_r), r, twin)

    def project(r):
        rows = pl.ds(r * ROWS, ROWS)
        mine = g[low, rows, :]
        both = jnp.concatenate([mine, g[1 - low, rows, :]], 0)
        made = dot(both, wkv[...]).astype(BF16)
        kv[kv_rows(2, r), :] = made[:ROWS]
        kv[kv_rows(other_slot, r), :] = made[ROWS:]

        @pl.when(has_next)
        def _():
            shift_line(r).start()

        @pl.when(core == 0)
        def _():
            to_twin(2, r).start()

        @pl.when(jnp.logical_and(core == 1, low == 1))
        def _():
            to_twin(0, r).start()

        q = dot(mine, wq[...]).astype(BF16).astype(F32)
        for h in range(4):
            cols = slice(h * HEAD, (h + 1) * HEAD)
            cq[r * ROWS : (r + 1) * ROWS, cols] = (q[:, cols] + bc[h : h + 1, :]).astype(BF16)
            pq[r * ROWS : (r + 1) * ROWS, cols] = (q[:, cols] + bp[h : h + 1, :]).astype(BF16)

    @pl.when(jnp.logical_and(front, s < 4))
    def _():
        kv[0:SEG, :] = jnp.zeros((SEG, 2 * WIDTH), BF16)

    rel[3 * SEG :, :] = jnp.zeros((ROWS, WIDTH), BF16)

    loads[0].wait()
    pl.semaphore_wait(barrier, 5)

    projected = False
    passed, made = 0, 0
    for _, way, p, d in gather_order():
        if way < 2:
            if d > 0:
                came(way, p, d).wait_recv()
            send(way, p, d).start()
            passed += 1
            if passed == 6:
                tables()
            if passed % 4 == 2 and passed > 8 and made < 6:
                if made == 0:
                    loads[1].wait()
                rel_rows(made)
                made += 1
            continue
        if not projected:
            for load in loads[2:5]:
                load.wait()
            projected = True
        for piece in range(p * ROWS // PIECE, (p + 1) * ROWS // PIECE):
            came(0, piece, REACH[0][piece]).wait_recv()
            came(1, piece, REACH[1][piece]).wait_recv()
        project(p)

    for r in range(CHUNKS):
        @pl.when(has_prev)
        def _():
            shift_line_in(r).wait_recv()

        @pl.when(jnp.logical_and(core == 1, front))
        def _():
            to_twin(0, r).start()

    for r in range(CHUNKS):
        to_twin(0, r).wait_recv()
    for load in loads[5:]:
        load.wait()

    start = jnp.maximum(2 * SEG - SEG * s, 0)
    scale = math.log2(math.e) / math.sqrt(HEAD)

    def attend(r):
        i0 = r * ROWS
        keys = 2 * SEG + ROWS + i0
        span = keys + ROWS
        e0 = SEG - ROWS - i0
        outside = jnp.where(lax.broadcasted_iota(jnp.int32, (1, keys), 1) >= start, 0.0, NEG).astype(F32)
        causal = lax.broadcasted_iota(jnp.int32, (ROWS, ROWS), 1) <= lax.broadcasted_iota(jnp.int32, (ROWS, ROWS), 0)

        def one(h):
            cols = slice(h * HEAD, (h + 1) * HEAD)
            vcols = slice(WIDTH + h * HEAD, WIDTH + (h + 1) * HEAD)
            content = dot_t(cq[i0 : i0 + ROWS, cols], kv[0:keys, cols])
            position = dot_t(pq[i0 : i0 + ROWS, cols], rel[e0 : e0 + span, cols])
            position = pltpu.roll(position, span - (ROWS - 1), 1, stride=1, stride_axis=0)[:, :keys]
            score = content + position + outside
            tail = jnp.where(causal, score[:, keys - ROWS :], NEG)
            score = jnp.concatenate([score[:, : keys - ROWS], tail], 1)
            top = jnp.max(score, axis=1, keepdims=True)
            e = jnp.exp2((score - top) * scale)
            norm = 1.0 / jnp.sum(e, axis=1, keepdims=True)
            att[i0 : i0 + ROWS, cols] = dot((e * norm).astype(BF16), kv[0:keys, vcols]).astype(BF16)

        for h in range(4):
            one(h)

    def opp_right(r):
        return copy_to(opp.at[r, pl.ds(0, HALF)], half_r.at[r], (or_s, or_r), r, to_right)

    def opp_left(r):
        return copy_to(opp.at[r, pl.ds(HALF, HALF)], half_l.at[r], (ol_s, ol_r), r, to_left)

    def fin_right(r, i):
        rows = pl.ds((1 - i) * HALF, HALF)
        return copy_to(near_r.at[r, rows], fin_r.at[r, rows], (fr_s, fr_r), (i, r), to_right)

    def fin_left(r, i):
        rows = pl.ds(i * HALF, HALF)
        return copy_to(near_l.at[r, rows], fin_l.at[r, rows], (fl_s, fl_r), (i, r), to_left)

    def output(r):
        a = att[r * ROWS : (r + 1) * ROWS, :]
        opp[r] = dot(a, wo[across]).astype(BF16)
        opp_right(r).start()
        opp_left(r).start()
        near_r[r] = dot(a, wo[right]).astype(BF16)
        fin_right(r, 0).start()
        near_l[r] = dot(a, wo[left]).astype(BF16)
        fin_left(r, 0).start()
        own[r] = dot(a, wo[t]).astype(BF16)

    def pass_on(r):
        opp_right(r).wait_recv()
        near_r[r, :HALF, :] = (near_r[r, :HALF, :].astype(F32) + half_r[r].astype(F32)).astype(BF16)
        fin_right(r, 1).start()
        opp_left(r).wait_recv()
        near_l[r, HALF:, :] = (near_l[r, HALF:, :].astype(F32) + half_l[r].astype(F32)).astype(BF16)
        fin_left(r, 1).start()

    others = (to_across, to_right, to_left)

    def stats_to(i, r):
        return copy_to(st_out.at[r], st_in.at[i, r], (st_s, st_r), (i, r), others[i])

    def collect(r):
        for i in range(2):
            fin_right(r, i).wait_recv()
            fin_left(r, i).wait_recv()
        rows = pl.ds(r * ROWS, ROWS)
        total = g[low, rows, own_cols].astype(F32) + (
            own[r].astype(F32) + fin_r[r].astype(F32) + fin_l[r].astype(F32)
        )
        y[r] = total
        mean = jnp.sum(total, axis=1, keepdims=True) * (1.0 / WIDTH)
        centred = total - mean
        square = jnp.sum(centred * centred, axis=1, keepdims=True)
        lane = lax.broadcasted_iota(jnp.int32, (ROWS, 128), 1)
        both = jnp.where(lane == 0, mean, jnp.where(lane == 1, square, 0.0))
        st_out[r] = both.T[:8, :]
        for i in range(3):
            stats_to(i, r).start()

    def finish(r):
        for i in range(3):
            stats_to(i, r).wait_recv()
        stack = jnp.concatenate(
            [st_out[r], st_in[0, r], st_in[1, r], st_in[2, r], jnp.zeros((96, 128), F32)], 0
        ).T
        means = [stack[:, 8 * i : 8 * i + 1] for i in range(4)]
        squares = [stack[:, 8 * i + 1 : 8 * i + 2] for i in range(4)]
        mean = (means[0] + means[1] + means[2] + means[3]) * 0.25
        square = squares[0] + squares[1] + squares[2] + squares[3]
        for m in means:
            square = square + WIDTH * ((m - mean) * (m - mean))
        factor = lax.rsqrt(square * (1.0 / MODEL) + 1e-05)
        normed = (y[r] - mean) * factor
        out[r * ROWS : (r + 1) * ROWS, :] = (normed * gain[...] + shift[...]).astype(BF16)

    for r in range(CHUNKS):
        attend(r)
        output(r)
        if r >= 1:
            pass_on(r - 1)
    pass_on(CHUNKS - 1)
    for r in range(CHUNKS):
        collect(r)
        if 1 <= r < CHUNKS - 1:
            finish(r - 1)
    finish(CHUNKS - 2)
    finish(CHUNKS - 1)

    for way in range(2):
        for p in range(PIECES):
            for d in range(REACH[way][p]):
                send(way, p, d).wait_send()
    for r in range(CHUNKS):
        @pl.when(has_next)
        def _():
            shift_line(r).wait_send()

        to_twin(0, r).wait_send()
        for copy in (opp_right(r), opp_left(r), fin_right(r, 0), fin_left(r, 0), fin_right(r, 1), fin_left(r, 1)):
            copy.wait_send()
        for i in range(3):
            stats_to(i, r).wait_send()


def layer(n_seq, hidden_in, w_query, w_key, w_value, w_pos, w_out, bias_content, bias_pos, norm_gain, norm_bias):
    anywhere = pl.BlockSpec(memory_space=pl.ANY)
    vmem = pl.BlockSpec(memory_space=pltpu.VMEM)
    dma = pltpu.SemaphoreType.DMA
    per_chunk = [dma((CHUNKS,))] * 2
    return pl.pallas_call(
        functools.partial(kernel, n_seq),
        out_shape=pltpu.VMEM((SEG, WIDTH), BF16),
        in_specs=[anywhere] * 6 + [vmem] * 4,
        out_specs=vmem,
        scratch_shapes=[
            pltpu.VMEM((2, SEG, MODEL), BF16),
            pltpu.VMEM((MODEL, WIDTH), BF16),
            pltpu.VMEM((MODEL, 2 * WIDTH), BF16),
            pltpu.VMEM((MODEL, WIDTH), BF16),
            pltpu.VMEM((4, WIDTH, WIDTH), BF16),
            pltpu.VMEM((4 * SEG, 2 * WIDTH), BF16),
            pltpu.VMEM((SEG, WIDTH), BF16),
            pltpu.VMEM((SEG, WIDTH), BF16),
            pltpu.VMEM((3 * SEG + ROWS, WIDTH), BF16),
            pltpu.VMEM((2, FINE, MODEL // 2), F32),
            pltpu.VMEM((2, 3 * SEG // FINE, MODEL // 2), F32),
            pltpu.VMEM((SEG, WIDTH), BF16),
            pltpu.VMEM((CHUNKS, ROWS, WIDTH), BF16),
            pltpu.VMEM((CHUNKS, ROWS, WIDTH), BF16),
            pltpu.VMEM((CHUNKS, ROWS, WIDTH), BF16),
            pltpu.VMEM((CHUNKS, ROWS, WIDTH), BF16),
            pltpu.VMEM((CHUNKS, HALF, WIDTH), BF16),
            pltpu.VMEM((CHUNKS, HALF, WIDTH), BF16),
            pltpu.VMEM((CHUNKS, ROWS, WIDTH), BF16),
            pltpu.VMEM((CHUNKS, ROWS, WIDTH), BF16),
            pltpu.VMEM((CHUNKS, ROWS, WIDTH), F32),
            pltpu.VMEM((CHUNKS, 8, 128), F32),
            pltpu.VMEM((3, CHUNKS, 8, 128), F32),
            dma((9,)),
            dma((4, PIECES)), dma((4, PIECES)), dma((4, PIECES)), dma((4, PIECES)),
            *per_chunk, *per_chunk, *per_chunk, *per_chunk,
            dma((2, CHUNKS)), dma((2, CHUNKS)), dma((2, CHUNKS)), dma((2, CHUNKS)),
            dma((3, CHUNKS)), dma((3, CHUNKS)),
        ],
        compiler_params=pltpu.CompilerParams(
            collective_id=0, has_side_effects=True, vmem_limit_bytes=66_200_000
        ),
    )(
        hidden_in, w_query, w_key, w_value, w_pos, w_out, bias_content, bias_pos,
        norm_gain.reshape(1, WIDTH), norm_bias.reshape(1, WIDTH),
    )


def solution(mesh):
    in_specs = (
        P("seq", "tp"),
        P(None, "tp"),
        P(None, "tp"),
        P(None, "tp"),
        P(None, "tp"),
        P("tp", None),
        P("tp", None),
        P("tp", None),
        P("tp"),
        P("tp"),
    )
    return jax.shard_map(
        functools.partial(layer, mesh.shape["seq"]),
        mesh=mesh,
        in_specs=in_specs,
        out_specs=P("seq", "tp"),
        check_vma=False,
    )
```
